32 devices in a mesh: mem: 8 (over z, x), head: 4 (over y, core).
Axes of the slice: x: 2, y: 2, z: 4, core: 2. Of those that a mesh axis runs over, the one named last changes fastest.
Arguments:
- queries: bfloat16 [128, 32, 128], P('mem', 'head'), may hold values from -170 to 170
- cache_blocks: bfloat16 [256, 2, 8, 64, 128], P('mem', None, 'head'), may hold values from -9 to 9
- selected: int32 [128, 32], P('mem'), may hold values from 0 to 255, as said below
- counts: int32 [16, 256], P(None, 'mem'), may hold values from 0 to 8
- output_weight: bfloat16 [4096, 4096], P('head'), may hold values from -0.09375 to 0.09375
Outputs:
- layer_out: bfloat16 [128, 4096], P('mem', 'head')
- block_heat: float32 [256], P('mem')
The draws below stay inside these ranges and needn't reach their ends.
Inputs may be any that keep to these rules, and one draw needn't show every extreme that they name: `selected`: each request names 32 different blocks; at most 8 of a request's blocks b share the same b // 32.
All inputs are finite; a program needn't handle non-finite values.
Results may differ from the reference program's by a relative error of at most 0.012.
Values may be sent and summed in bfloat16 or wider, within the bound.
No kernel may reach another device: no remote copies, remote signals or barrier semaphores. Data moves between devices by JAX's collectives and lax.ppermute only.
A program may use at most 128 MiB of HBM per device.

```python
import jax
import jax.numpy as jnp
from jax import lax

D = 4096
QUERY_HEADS = 32
KEY_VALUE_HEADS = 8
HEAD_SIZE = 128
BLOCK_TOKENS = 64
SEL = 32
HIST = 16
BLK_DEV = 32
MOST = 8
REQUESTS = 128
TOTAL_KV_BLOCKS = 256
N_MEM = 8


def pick_blocks(key):
    k_hot, k_pool, k_within, k_order = jax.random.split(key, 4)
    hot_device = jax.random.randint(k_hot, (), 0, N_MEM).astype(jnp.int32)
    others = (hot_device + 1 + jnp.arange(N_MEM - 1, dtype=jnp.int32)) % N_MEM
    candidates = jnp.tile(others, MOST)
    spread = candidates.shape[0]
    shuffled = jax.random.randint(k_pool, (REQUESTS, spread), 0, 1 << 20) * spread + jnp.arange(spread, dtype=jnp.int32)[None, :]
    ordering = jnp.argsort(shuffled, axis=1)
    remaining = candidates[ordering[:, :SEL - MOST]]
    target = jnp.concatenate([jnp.full((REQUESTS, MOST), hot_device, jnp.int32), remaining], axis=1)
    onehot = (target[:, :, None] == jnp.arange(N_MEM, dtype=jnp.int32)[None, None, :]).astype(jnp.int32)
    ranking = jnp.sum((jnp.cumsum(onehot, axis=1) - onehot) * onehot, axis=2)
    inner_keys = jax.random.randint(k_within, (REQUESTS, N_MEM, BLK_DEV), 0, 1 << 20) * BLK_DEV + jnp.arange(BLK_DEV, dtype=jnp.int32)
    within = jnp.argsort(inner_keys, axis=2).astype(jnp.int32)
    chosen = within[jnp.arange(REQUESTS)[:, None], target, ranking]
    block_ids = target * BLK_DEV + chosen
    final_keys = jax.random.randint(k_order, (REQUESTS, SEL), 0, 1 << 20) * SEL + jnp.arange(SEL, dtype=jnp.int32)[None, :]
    return jnp.take_along_axis(block_ids, jnp.argsort(final_keys, axis=1), axis=1).astype(jnp.int32)


def cache_values(key):
    value_vectors = jax.random.truncated_normal(key, -4.5, 4.5, (TOTAL_KV_BLOCKS, 2, KEY_VALUE_HEADS, BLOCK_TOKENS, HEAD_SIZE), jnp.float32)
    return value_vectors


def draw_selected(key, part):
    return pick_blocks(jax.random.fold_in(key, 7))


def draw_cache_blocks(key, part):
    return cache_values(jax.random.fold_in(key, 11)).astype(jnp.bfloat16)


def draw_queries(key, part):
    value_vectors = jax.random.truncated_normal(jax.random.fold_in(key, 3), -4.5, 4.5, (REQUESTS, QUERY_HEADS, HEAD_SIZE), jnp.float32)
    return value_vectors.astype(jnp.bfloat16)


def place_ends(drawn, stream_key, low, high):
    spot = [jax.random.randint(jax.random.fold_in(stream_key, axis), (), 0, length) for axis, length in enumerate(drawn.shape)]
    longest = drawn.shape.index(max(drawn.shape))
    beside = spot[:longest] + [(spot[longest] + 1) % drawn.shape[longest]] + spot[longest + 1:]
    return drawn.at[tuple(spot)].set(low).at[tuple(beside)].set(high)


def block_levels(key, dims, cuts, low, top_value):
    factor_of = 1.0
    for axis_at, shards_of in cuts:
        heights = jax.random.uniform(jax.random.fold_in(jax.random.fold_in(key, 6), axis_at), (shards_of,), jnp.float32, low / len(cuts), top_value / len(cuts))
        factor_of = factor_of * jnp.repeat(jnp.exp(heights), dims[axis_at] // shards_of).reshape((-1,) + (1,) * (len(dims) - 1 - axis_at))
    return factor_of


def noise(rng, dims, scale, reach, cuts=(), held_as=jnp.bfloat16):
    values = jax.random.normal(rng, dims, jnp.float32) * scale
    if len(cuts) > 0:
        values = block_levels(rng, dims, cuts, -0.22, 0.18) * values
    return jnp.clip(values, min=-reach, max=reach).astype(held_as)


def setup_inputs(seed: int = 0) -> dict:
    key_list = jax.random.split(jax.random.key(seed), 6)
    return {
        "queries": draw_queries(jax.random.fold_in(key_list[5], 71), 0),
        "cache_blocks": draw_cache_blocks(jax.random.fold_in(key_list[5], 71), 0),
        "selected": draw_selected(jax.random.fold_in(key_list[5], 71), 0),
        "counts": place_ends(jax.random.randint(key_list[3], (HIST, TOTAL_KV_BLOCKS), 0, 9), jax.random.fold_in(key_list[3], 1), 0, 8).astype(jnp.int32),
        "output_weight": noise(key_list[4], (QUERY_HEADS * HEAD_SIZE, D), (QUERY_HEADS * HEAD_SIZE) ** -0.5, 0.09375, ((0, 4),)),
    }


def block_partial(single_query_row, key_rows, value_rows):
    group_stacked = single_query_row.astype(jnp.float32).reshape(KEY_VALUE_HEADS, QUERY_HEADS // KEY_VALUE_HEADS, HEAD_SIZE)
    scores = jnp.einsum("hgd,htd->hgt", group_stacked, key_rows.astype(jnp.float32)) * (HEAD_SIZE ** -0.5)
    peak_score = jnp.max(scores, axis=-1)
    expo_terms = jnp.exp(scores - peak_score[..., None])
    totals = jnp.sum(expo_terms, axis=-1)
    weights = lax.optimization_barrier(expo_terms.astype(jnp.bfloat16)).astype(jnp.float32)
    outputs = jnp.einsum("hgt,htd->hgd", weights, value_rows.astype(jnp.float32))
    return peak_score, totals, outputs


def reference(queries, cache_blocks, selected, counts, output_weight):
    def one_request(inputs):
        single_query_row, chosen = inputs
        blocks = cache_blocks[chosen]
        peak_score, totals, outputs = jax.vmap(block_partial, in_axes=(None, 0, 0))(single_query_row, blocks[:, 0], blocks[:, 1])
        highest = jnp.max(peak_score, axis=0)
        factor = jnp.exp(peak_score - highest)
        denominator = jnp.sum(factor * totals, axis=0)
        numerator = jnp.sum(factor[..., None] * outputs, axis=0)
        return (numerator / denominator[..., None]).reshape(QUERY_HEADS * HEAD_SIZE).astype(jnp.bfloat16)

    attended = lax.map(one_request, (queries, selected))
    layer_out = jnp.dot(attended, output_weight, preferred_element_type=jnp.float32).astype(jnp.bfloat16)
    access_hits = jnp.zeros((TOTAL_KV_BLOCKS,), jnp.float32).at[selected.reshape(-1)].add(1.0)
    decays = 0.5 ** jnp.arange(HIST, dtype=jnp.float32)
    block_heat = jnp.sum(decays[:, None] * counts.astype(jnp.float32), axis=0) + access_hits
    return layer_out, block_heat
```

```python
import functools
import math

import jax
import jax.numpy as jnp
from jax import lax
from jax.experimental import pallas as pl
from jax.experimental.pallas import tpu as pltpu
from jax.sharding import PartitionSpec as P

MASKED = -1e30
LANES = 128


def nt_dot(left, right):
    return lax.dot_general(
        left, right, (((1,), (1,)), ((), ())), preferred_element_type=jnp.float32
    )


def attend_kernel(index_ref, *refs, sources, heads, heads_kv, rows_each):
    payloads = refs[:sources]
    cache_ref, counts_ref = refs[sources : sources + 2]
    messages = refs[sources + 2 : 2 * sources + 2]
    heat_ref = refs[2 * sources + 2]
    blocks, _, _, tokens, depth = cache_ref.shape
    width = heads * depth
    all_blocks = payloads[0].shape[1] - width
    group_q = heads // heads_kv
    scale = depth**-0.5 * math.log2(math.e)
    first = index_ref[0] * blocks
    pick = (
        lax.broadcasted_iota(jnp.int32, (all_blocks, LANES), 0)
        == lax.broadcasted_iota(jnp.int32, (all_blocks, LANES), 1) + first
    ) & (lax.broadcasted_iota(jnp.int32, (all_blocks, LANES), 1) < blocks)
    pick = pick.astype(jnp.float32).astype(jnp.bfloat16)
    span = blocks * tokens
    fence = jnp.where(
        lax.broadcasted_iota(jnp.int32, (span, LANES), 0) // tokens
        == lax.broadcasted_iota(jnp.int32, (span, LANES), 1),
        MASKED,
        0.0,
    ).astype(jnp.bfloat16)
    hits = jnp.zeros((1, LANES), jnp.float32)
    batch = min(sources, 8)
    rows = batch * rows_each
    lane = lax.broadcasted_iota(jnp.int32, (rows, LANES), 1)
    for start in range(0, sources, batch):
        part = payloads[start : start + batch]
        marks = jnp.concatenate([p[:, width:] for p in part], axis=0)
        chosen = jnp.dot(marks, pick, preferred_element_type=jnp.float32)
        hits = hits + jnp.sum(chosen, axis=0, keepdims=True)
        blocked = (1.0 - chosen).astype(jnp.bfloat16)
        stats = jnp.zeros((rows, LANES), jnp.float32)
        for kv in range(heads_kv):
            keys = cache_ref[:, 0, kv].reshape(span, depth)
            keys = jnp.concatenate([keys, fence], axis=1)
            values = cache_ref[:, 1, kv].reshape(span, depth)
            for g in range(group_q):
                h = kv * group_q + g
                query = jnp.concatenate([p[:, h * depth : (h + 1) * depth] for p in part], axis=0)
                query = jnp.concatenate([query, blocked], axis=1)
                scores = nt_dot(query, keys)
                peak = jnp.max(scores, axis=1, keepdims=True)
                weights = jnp.exp2((scores - peak) * scale)
                total = jnp.sum(weights, axis=1, keepdims=True)
                out = jnp.dot(
                    weights.astype(jnp.bfloat16), values, preferred_element_type=jnp.float32
                ).astype(jnp.bfloat16)
                for i in range(batch):
                    messages[start + i][:, h * depth : (h + 1) * depth] = out[
                        i * rows_each : (i + 1) * rows_each
                    ]
                stats = jnp.where(lane == h, peak, stats)
                stats = jnp.where(lane == heads + h, total, stats)
        high = stats.astype(jnp.bfloat16).astype(jnp.float32)
        rest = stats - high
        middle = rest.astype(jnp.bfloat16).astype(jnp.float32)
        low = rest - middle
        packed = (
            high + pltpu.roll(middle, 2 * heads, 1) + pltpu.roll(low, 4 * heads, 1)
        ).astype(jnp.bfloat16)
        for i in range(batch):
            messages[start + i][:, width:] = packed[i * rows_each : (i + 1) * rows_each]
    history = counts_ref.shape[0]
    steps = lax.broadcasted_iota(jnp.int32, counts_ref.shape, 0).astype(jnp.float32)
    decayed = jnp.sum(
        jnp.exp2(-steps) * counts_ref[...].astype(jnp.float32), axis=0, keepdims=True
    )
    heat_ref[...] = decayed + hits[:, :blocks]


def project_kernel(*refs, sources, heads):
    messages = refs[:sources]
    weight_ref = refs[sources]
    outs = refs[sources + 1 :]
    rows = messages[0].shape[0]
    width = weight_ref.shape[0]
    depth = width // heads
    scale = depth**-0.5 * math.log2(math.e)
    stats = []
    for m in messages:
        packed = m[:, width:].astype(jnp.float32)
        stats.append(
            packed
            + pltpu.roll(packed, LANES - 2 * heads, 1)
            + pltpu.roll(packed, LANES - 4 * heads, 1)
        )
    lane = lax.broadcasted_iota(jnp.int32, (rows, LANES), 1)
    highest = functools.reduce(jnp.maximum, stats)
    factors = [jnp.where(lane < heads, jnp.exp2((s - highest) * scale), 0.0) for s in stats]
    total = sum(f * pltpu.roll(s, LANES - heads, 1) for f, s in zip(factors, stats))
    inverse = 1.0 / jnp.where(lane < heads, total, 1.0)
    factors = [f * inverse for f in factors]
    attended = []
    for h in range(heads):
        acc = None
        for f, m in zip(factors, messages):
            term = f[:, h : h + 1] * m[:, h * depth : (h + 1) * depth].astype(jnp.float32)
            acc = term if acc is None else acc + term
        attended.append(acc.astype(jnp.bfloat16))
    attended = jnp.concatenate(attended, axis=1)
    columns = weight_ref.shape[1] // len(outs)
    for i, out in enumerate(outs):
        out[...] = jnp.dot(
            attended,
            weight_ref[:, i * columns : (i + 1) * columns],
            preferred_element_type=jnp.float32,
        ).astype(jnp.bfloat16)


def per_device(queries, cache_blocks, selected, counts, output_weight):
    devices_mem = lax.axis_size("mem")
    devices_head = lax.axis_size("head")
    rows, heads, depth = queries.shape
    blocks, _, heads_kv, tokens, _ = cache_blocks.shape
    width = heads * depth
    all_blocks = devices_mem * blocks
    marks = jnp.any(
        selected[:, :, None] == jnp.arange(all_blocks, dtype=jnp.int32)[None, None, :], axis=1
    ).astype(jnp.bfloat16)
    payload = jnp.concatenate([queries.reshape(rows, width), marks], axis=1)
    payloads = [payload] + [
        lax.ppermute(payload, "mem", [(i, (i + k) % devices_mem) for i in range(devices_mem)])
        for k in range(1, devices_mem)
    ]
    vmem = pl.BlockSpec(memory_space=pltpu.VMEM)
    message_shape = jax.ShapeDtypeStruct((rows, width + LANES), jnp.bfloat16)
    index = lax.axis_index("mem").astype(jnp.int32).reshape(1)
    *messages, heat = pl.pallas_call(
        functools.partial(
            attend_kernel, sources=devices_mem, heads=heads, heads_kv=heads_kv, rows_each=rows
        ),
        in_specs=[pl.BlockSpec(memory_space=pltpu.SMEM)] + [vmem] * (devices_mem + 2),
        out_specs=[vmem] * (devices_mem + 1),
        out_shape=[message_shape] * devices_mem
        + [jax.ShapeDtypeStruct((1, blocks), jnp.float32)],
        compiler_params=pltpu.CompilerParams(vmem_limit_bytes=40 * 2**20),
        name="attend",
    )(index, *payloads, cache_blocks, counts)
    returned = [messages[0]] + [
        lax.ppermute(
            messages[k], "mem", [(i, (i - k) % devices_mem) for i in range(devices_mem)]
        )
        for k in range(1, devices_mem)
    ]
    me = lax.axis_index("head")
    columns = output_weight.shape[1] // devices_head
    shares = pl.pallas_call(
        functools.partial(project_kernel, sources=devices_mem, heads=heads),
        in_specs=[vmem] * (devices_mem + 1),
        out_specs=[vmem] * devices_head,
        out_shape=[jax.ShapeDtypeStruct((rows, columns), jnp.bfloat16)] * devices_head,
        compiler_params=pltpu.CompilerParams(vmem_limit_bytes=24 * 2**20),
        name="project",
    )(*returned, output_weight)
    shares = jnp.stack(shares)
    layer_out = None
    for k in range(devices_head):
        share = lax.dynamic_index_in_dim(shares, (me + k) % devices_head, 0, keepdims=False)
        if k:
            share = lax.ppermute(
                share, "head", [(i, (i + k) % devices_head) for i in range(devices_head)]
            )
        share = share.astype(jnp.float32)
        layer_out = share if layer_out is None else layer_out + share
    return (layer_out.astype(jnp.bfloat16), heat.reshape(blocks))


def solution(mesh):
    return jax.shard_map(
        per_device,
        mesh=mesh,
        in_specs=(
            P("mem", "head", None),
            P("mem", None, "head", None, None),
            P("mem", None),
            P(None, "mem"),
            P("head", None),
        ),
        out_specs=(P("mem", "head"), P("mem")),
        check_vma=False,
    )
```

```python
import functools
import math

import jax
import jax.numpy as jnp
from jax import lax
from jax.experimental import pallas as pl
from jax.experimental.pallas import tpu as pltpu
from jax.sharding import PartitionSpec as P


MASKED = -1e30
LANES = 128


def exchange(value, axis, step):
    count = lax.axis_size(axis)
    return lax.ppermute(value, axis, [(i, i ^ step) for i in range(count)])


def payload_kernel(queries_hbm, selected_hbm, out_ref, queries_ref, selected_ref, sems):
    copies = [
        pltpu.make_async_copy(selected_hbm, selected_ref, sems.at[0]),
        pltpu.make_async_copy(queries_hbm, queries_ref, sems.at[1]),
    ]
    for copy in copies:
        copy.start()
    rows, heads, depth = queries_ref.shape
    width = heads * depth
    block = lax.broadcasted_iota(jnp.int32, (rows, out_ref.shape[1] - width), 1)
    marks = jnp.zeros(block.shape, jnp.float32)
    copies[0].wait()
    chosen = selected_ref[...]
    for i in range(chosen.shape[1]):
        marks = jnp.where(block == chosen[:, i : i + 1], 1.0, marks)
    out_ref[:, width:] = marks.astype(jnp.bfloat16)
    copies[1].wait()
    for h in range(heads):
        out_ref[:, h * depth : (h + 1) * depth] = queries_ref[:, h, :]


def stage_kernel(source_hbm, _, out_ref, sem):
    copy = pltpu.make_async_copy(source_hbm, out_ref, sem)
    copy.start()
    copy.wait()


def attend_kernel(own_ref, near_ref, straight_ref, forwarded_ref, cache_ref, *refs, heads):
    messages = refs[:-1]
    hits_ref = refs[-1]
    blocks, _, heads_kv, tokens, depth = cache_ref.shape
    width = heads * depth
    rows_each = own_ref.shape[0]
    all_blocks = own_ref.shape[1] - width
    group_q = heads // heads_kv
    scale = depth**-0.5 * math.log2(math.e)
    payloads = [own_ref, near_ref]
    payloads += [straight_ref.at[i] for i in range(straight_ref.shape[0])]
    payloads += [forwarded_ref.at[i] for i in range(forwarded_ref.shape[0])]
    first = lax.axis_index("mem") * blocks
    column = lax.broadcasted_iota(jnp.int32, (all_blocks, LANES), 1)
    pick = (lax.broadcasted_iota(jnp.int32, (all_blocks, LANES), 0) == column + first) & (
        column < blocks
    )
    pick = pick.astype(jnp.float32).astype(jnp.bfloat16)
    span = blocks * tokens
    fence = jnp.where(
        lax.broadcasted_iota(jnp.int32, (span, LANES), 0) // tokens
        == lax.broadcasted_iota(jnp.int32, (span, LANES), 1),
        MASKED,
        0.0,
    ).astype(jnp.bfloat16)
    hits = jnp.zeros((1, LANES), jnp.float32)
    batch = min(len(payloads), 8)
    pair = math.gcd(group_q, 2)
    rows = batch * rows_each
    lane = lax.broadcasted_iota(jnp.int32, (rows, LANES), 1)
    for start in range(0, len(payloads), batch):
        part = payloads[start : start + batch]
        marks = jnp.concatenate([p[:, width:] for p in part], axis=0)
        chosen = jnp.dot(marks, pick, preferred_element_type=jnp.float32)
        hits = hits + jnp.sum(chosen, axis=0, keepdims=True)
        blocked = (1.0 - chosen).astype(jnp.bfloat16)
        stats = jnp.zeros((rows, LANES), jnp.float32)
        for kv in range(heads_kv):
            keys = cache_ref[:, 0, kv].reshape(span, depth)
            keys = jnp.concatenate([keys, fence], axis=1)
            values = cache_ref[:, 1, kv].reshape(span, depth)
            values = jnp.concatenate([values, jnp.ones((span, LANES), jnp.bfloat16)], axis=1)
            for first_head in range(kv * group_q, (kv + 1) * group_q, pair):
                query = jnp.concatenate(
                    [
                        jnp.concatenate(
                            [
                                jnp.concatenate(
                                    [p[:, h * depth : (h + 1) * depth] for p in part], axis=0
                                ),
                                blocked,
                            ],
                            axis=1,
                        )
                        for h in range(first_head, first_head + pair)
                    ],
                    axis=0,
                )
                scores = lax.dot_general(
                    query, keys, (((1,), (1,)), ((), ())), preferred_element_type=jnp.float32
                )
                peak = jnp.max(scores, axis=1, keepdims=True)
                weights = jnp.exp2((scores - peak) * scale).astype(jnp.bfloat16)
                sums = jnp.dot(weights, values, preferred_element_type=jnp.float32)
                out = sums[:, :depth].astype(jnp.bfloat16)
                total = sums[:, depth : depth + 1]
                for j in range(pair):
                    h = first_head + j
                    for i in range(batch):
                        at = j * rows + i * rows_each
                        messages[start + i][:, h * depth : (h + 1) * depth] = out[
                            at : at + rows_each
                        ]
                    stats = jnp.where(lane == h, peak[j * rows : (j + 1) * rows], stats)
                    stats = jnp.where(lane == heads + h, total[j * rows : (j + 1) * rows], stats)
        high = stats.astype(jnp.bfloat16).astype(jnp.float32)
        rest = stats - high
        middle = rest.astype(jnp.bfloat16).astype(jnp.float32)
        low = rest - middle
        packed = (
            high + pltpu.roll(middle, 2 * heads, 1) + pltpu.roll(low, 4 * heads, 1)
        ).astype(jnp.bfloat16)
        for i in range(batch):
            messages[start + i][:, width:] = packed[i * rows_each : (i + 1) * rows_each]
    hits_ref[...] = hits


def project_kernel(*refs, sources, heads):
    messages = refs[:sources]
    weight_ref = refs[sources]
    outs = refs[sources + 1 :]
    me = lax.axis_index("head")
    rows = messages[0].shape[0]
    width = weight_ref.shape[0]
    depth = width // heads
    scale = depth**-0.5 * math.log2(math.e)
    stats = []
    for m in messages:
        packed = m[:, width:].astype(jnp.float32)
        stats.append(
            packed
            + pltpu.roll(packed, LANES - 2 * heads, 1)
            + pltpu.roll(packed, LANES - 4 * heads, 1)
        )
    lane = lax.broadcasted_iota(jnp.int32, (rows, LANES), 1)
    highest = functools.reduce(jnp.maximum, stats)
    factors = [jnp.where(lane < heads, jnp.exp2((s - highest) * scale), 0.0) for s in stats]
    total = sum(f * pltpu.roll(s, LANES - heads, 1) for f, s in zip(factors, stats))
    inverse = 1.0 / jnp.where(lane < heads, total, 1.0)
    factors = [f * inverse for f in factors]
    attended = []
    for h in range(heads):
        acc = None
        for f, m in zip(factors, messages):
            term = f[:, h : h + 1] * m[:, h * depth : (h + 1) * depth].astype(jnp.float32)
            acc = term if acc is None else acc + term
        attended.append(acc.astype(jnp.bfloat16))
    attended = jnp.concatenate(attended, axis=1)
    columns = weight_ref.shape[1] // len(outs)
    for i, out in enumerate(outs):
        at = pl.multiple_of((me ^ i) * columns, columns)
        out[...] = jnp.dot(
            attended, weight_ref[:, pl.ds(at, columns)], preferred_element_type=jnp.float32
        ).astype(jnp.bfloat16)


def per_device(queries, cache_blocks, selected, counts, output_weight):
    devices_mem = lax.axis_size("mem")
    devices_head = lax.axis_size("head")
    rows, heads, depth = queries.shape
    blocks = cache_blocks.shape[0]
    width = heads * depth
    all_blocks = devices_mem * blocks
    vmem = pl.BlockSpec(memory_space=pltpu.VMEM)
    hbm = pl.BlockSpec(memory_space=pltpu.HBM)
    keep = functools.partial(pltpu.with_memory_space_constraint, memory_space=pltpu.HBM)
    payload = pl.pallas_call(
        payload_kernel,
        in_specs=[hbm] * 2,
        out_specs=vmem,
        out_shape=jax.ShapeDtypeStruct((rows, width + all_blocks), jnp.bfloat16),
        scratch_shapes=[
            pltpu.VMEM(queries.shape, queries.dtype),
            pltpu.VMEM(selected.shape, selected.dtype),
            pltpu.SemaphoreType.DMA((2,)),
        ],
        compiler_params=pltpu.CompilerParams(vmem_limit_bytes=4 * 2**20),
        name="payload",
    )(keep(queries), keep(selected))

    def stage(array, after):
        return pl.pallas_call(
            stage_kernel,
            in_specs=[hbm, vmem],
            out_specs=vmem,
            out_shape=jax.ShapeDtypeStruct(array.shape, array.dtype),
            scratch_shapes=[pltpu.SemaphoreType.DMA(())],
            compiler_params=pltpu.CompilerParams(vmem_limit_bytes=4 * 2**20),
        )(keep(array), after)

    even = list(range(devices_mem - 2, 0, -2))
    straight = jnp.stack([exchange(payload, "mem", k) for k in even])
    near = exchange(payload, "mem", 1)
    cache_blocks = stage(cache_blocks, payload)
    forwarded = exchange(straight, "mem", 1)
    output_weight = stage(output_weight, straight)
    steps = [0, 1] + even + [k ^ 1 for k in even]
    message_shape = jax.ShapeDtypeStruct((rows, width + LANES), jnp.bfloat16)
    *messages, hits = pl.pallas_call(
        functools.partial(attend_kernel, heads=heads),
        in_specs=[vmem] * 5,
        out_specs=[vmem] * (devices_mem + 1),
        out_shape=[message_shape] * devices_mem + [jax.ShapeDtypeStruct((1, LANES), jnp.float32)],
        compiler_params=pltpu.CompilerParams(vmem_limit_bytes=32 * 2**20),
        name="attend",
    )(payload, near, straight, forwarded, cache_blocks)
    returned = [m if k == 0 else exchange(m, "mem", k) for k, m in zip(steps, messages)]
    columns = output_weight.shape[1] // devices_head
    shares = pl.pallas_call(
        functools.partial(project_kernel, sources=devices_mem, heads=heads),
        in_specs=[vmem] * (devices_mem + 1),
        out_specs=[vmem] * devices_head,
        out_shape=[jax.ShapeDtypeStruct((rows, columns), jnp.bfloat16)] * devices_head,
        compiler_params=pltpu.CompilerParams(vmem_limit_bytes=24 * 2**20),
        name="project",
    )(*returned, output_weight)
    arrived = {k: exchange(shares[k], "head", k) for k in range(devices_head - 1, 0, -1)}
    layer_out = shares[0].astype(jnp.float32)
    for k in range(1, devices_head):
        layer_out = layer_out + arrived[k].astype(jnp.float32)
    decays = 0.5 ** jnp.arange(counts.shape[0], dtype=jnp.float32)
    block_heat = jnp.sum(decays[:, None] * counts.astype(jnp.float32), axis=0) + hits[0, :blocks]
    return (layer_out.astype(jnp.bfloat16), block_heat)


def solution(mesh):
    return jax.shard_map(
        per_device,
        mesh=mesh,
        in_specs=(
            P("mem", "head", None),
            P("mem", None, "head", None, None),
            P("mem", None),
            P(None, "mem"),
            P("head", None),
        ),
        out_specs=(P("mem", "head"), P("mem")),
        check_vma=False,
    )
```

```python
import functools
import math

import jax
import jax.numpy as jnp
from jax import lax
from jax.experimental import pallas as pl
from jax.experimental.pallas import tpu as pltpu
from jax.sharding import PartitionSpec as P


MASKED = -1e30
LANES = 128


def exchange(value, axis, step):
    count = lax.axis_size(axis)
    return lax.ppermute(value, axis, [(i, i ^ step) for i in range(count)])


def split_stats(stats, heads):
    high = stats.astype(jnp.bfloat16).astype(jnp.float32)
    rest = stats - high
    middle = rest.astype(jnp.bfloat16).astype(jnp.float32)
    low = rest - middle
    packed = high + pltpu.roll(middle, 2 * heads, 1) + pltpu.roll(low, 4 * heads, 1)
    return packed.astype(jnp.bfloat16)


def join_stats(packed, heads):
    packed = packed.astype(jnp.float32)
    return (
        packed
        + pltpu.roll(packed, LANES - 2 * heads, 1)
        + pltpu.roll(packed, LANES - 4 * heads, 1)
    )


def merge_partials(messages, heads, width):
    depth = width // heads
    scale = depth**-0.5 * math.log2(math.e)
    stats = [join_stats(m[:, width:], heads) for m in messages]
    lane = lax.broadcasted_iota(jnp.int32, stats[0].shape, 1)
    highest = functools.reduce(jnp.maximum, stats)
    factors = [jnp.where(lane < heads, jnp.exp2((s - highest) * scale), 0.0) for s in stats]
    total = sum(f * pltpu.roll(s, LANES - heads, 1) for f, s in zip(factors, stats))
    return highest, total, factors, lane


def weighted_sums(messages, factors, heads, depth):
    for h in range(heads):
        acc = None
        for f, m in zip(factors, messages):
            term = f[:, h : h + 1] * m[:, h * depth : (h + 1) * depth].astype(jnp.float32)
            acc = term if acc is None else acc + term
        yield h, acc.astype(jnp.bfloat16)


def payload_kernel(queries_hbm, selected_hbm, out_ref, queries_ref, selected_ref, sems):
    copies = [
        pltpu.make_async_copy(selected_hbm, selected_ref, sems.at[0]),
        pltpu.make_async_copy(queries_hbm, queries_ref, sems.at[1]),
    ]
    for copy in copies:
        copy.start()
    rows, heads, depth = queries_ref.shape
    width = heads * depth
    block = lax.broadcasted_iota(jnp.int32, (rows, out_ref.shape[1] - width), 1)
    marks = jnp.zeros(block.shape, jnp.float32)
    copies[0].wait()
    chosen = selected_ref[...]
    for i in range(chosen.shape[1]):
        marks = jnp.where(block == chosen[:, i : i + 1], 1.0, marks)
    out_ref[:, width:] = marks.astype(jnp.bfloat16)
    copies[1].wait()
    for h in range(heads):
        out_ref[:, h * depth : (h + 1) * depth] = queries_ref[:, h, :]


def stage_kernel(source_hbm, _, out_ref, sem):
    copy = pltpu.make_async_copy(source_hbm, out_ref, sem)
    copy.start()
    copy.wait()


def attend_kernel(single_ref, several_ref, cache_ref, messages_ref, hits_ref, *, heads):
    blocks, _, heads_kv, tokens, depth = cache_ref.shape
    width = heads * depth
    rows_each = single_ref.shape[0]
    all_blocks = single_ref.shape[1] - width
    group_q = heads // heads_kv
    scale = depth**-0.5 * math.log2(math.e)
    payloads = [single_ref] + [several_ref.at[i] for i in range(several_ref.shape[0])]
    first = lax.axis_index("mem") * blocks
    column = lax.broadcasted_iota(jnp.int32, (all_blocks, LANES), 1)
    pick = (lax.broadcasted_iota(jnp.int32, (all_blocks, LANES), 0) == column + first) & (
        column < blocks
    )
    pick = pick.astype(jnp.float32).astype(jnp.bfloat16)
    span = blocks * tokens
    fence = jnp.where(
        lax.broadcasted_iota(jnp.int32, (span, LANES), 0) // tokens
        == lax.broadcasted_iota(jnp.int32, (span, LANES), 1),
        MASKED,
        0.0,
    ).astype(jnp.bfloat16)
    hits = jnp.zeros((1, LANES), jnp.float32)
    batch = min(len(payloads), 8)
    pair = math.gcd(group_q, max(1, 256 // (batch * rows_each)))
    rows = batch * rows_each
    lane = lax.broadcasted_iota(jnp.int32, (rows, LANES), 1)
    for start in range(0, len(payloads), batch):
        part = payloads[start : start + batch]
        marks = jnp.concatenate([p[:, width:] for p in part], axis=0)
        chosen = jnp.dot(marks, pick, preferred_element_type=jnp.float32)
        hits = hits + jnp.sum(chosen, axis=0, keepdims=True)
        blocked = (1.0 - chosen).astype(jnp.bfloat16)
        stats = jnp.zeros((rows, LANES), jnp.float32)
        for kv in range(heads_kv):
            keys = cache_ref[:, 0, kv].reshape(span, depth)
            keys = jnp.concatenate([keys, fence], axis=1)
            values = cache_ref[:, 1, kv].reshape(span, depth)
            values = jnp.concatenate([values, jnp.ones((span, LANES), jnp.bfloat16)], axis=1)
            for first_head in range(kv * group_q, (kv + 1) * group_q, pair):
                query = jnp.concatenate(
                    [
                        jnp.concatenate(
                            [
                                jnp.concatenate(
                                    [p[:, h * depth : (h + 1) * depth] for p in part], axis=0
                                ),
                                blocked,
                            ],
                            axis=1,
                        )
                        for h in range(first_head, first_head + pair)
                    ],
                    axis=0,
                )
                scores = lax.dot_general(
                    query, keys, (((1,), (1,)), ((), ())), preferred_element_type=jnp.float32
                )
                peak = jnp.max(scores, axis=1, keepdims=True)
                weights = jnp.exp2((scores - peak) * scale).astype(jnp.bfloat16)
                sums = jnp.dot(weights, values, preferred_element_type=jnp.float32)
                out = sums[:, :depth].astype(jnp.bfloat16)
                total = sums[:, depth : depth + 1]
                for j in range(pair):
                    h = first_head + j
                    for i in range(batch):
                        at = j * rows + i * rows_each
                        messages_ref[start + i, :, h * depth : (h + 1) * depth] = out[
                            at : at + rows_each
                        ]
                    stats = jnp.where(lane == h, peak[j * rows : (j + 1) * rows], stats)
                    stats = jnp.where(lane == heads + h, total[j * rows : (j + 1) * rows], stats)
        packed = split_stats(stats, heads)
        for i in range(batch):
            messages_ref[start + i, :, width:] = packed[i * rows_each : (i + 1) * rows_each]
    hits_ref[...] = hits


def merge_kernel(mine_ref, theirs_ref, *outs, heads):
    width = mine_ref.shape[2] - LANES
    depth = width // heads
    for i, out in enumerate(outs):
        pair = [mine_ref.at[i], theirs_ref.at[i]]
        highest, total, factors, lane = merge_partials(pair, heads, width)
        for h, merged in weighted_sums(pair, factors, heads, depth):
            out[:, h * depth : (h + 1) * depth] = merged
        stats = jnp.where(lane < heads, highest, pltpu.roll(total, heads, 1))
        stats = jnp.where(lane < 2 * heads, stats, 0.0)
        out[:, width:] = split_stats(stats, heads)


def project(attended, weight_ref, steps, outs):
    me = lax.axis_index("head")
    columns = outs[0].shape[1]
    for k, out in zip(steps, outs):
        at = pl.multiple_of((me ^ k) * columns, columns)
        out[...] = jnp.dot(
            attended, weight_ref[:, pl.ds(at, columns)], preferred_element_type=jnp.float32
        ).astype(jnp.bfloat16)


def project_far_kernel(*refs, sources, heads, steps):
    messages = refs[:sources]
    weight_ref, attended_ref = refs[sources : sources + 2]
    outs = refs[sources + 2 :]
    width = attended_ref.shape[1]
    depth = width // heads
    _, total, factors, lane = merge_partials(messages, heads, width)
    inverse = 1.0 / jnp.where(lane < heads, total, 1.0)
    factors = [f * inverse for f in factors]
    attended = jnp.concatenate(
        [a for _, a in weighted_sums(messages, factors, heads, depth)], axis=1
    )
    attended_ref[...] = attended
    project(attended, weight_ref, steps, outs)


def project_near_kernel(attended_ref, weight_ref, *outs, steps):
    project(attended_ref[...], weight_ref, steps, outs)


def per_device(queries, cache_blocks, selected, counts, output_weight):
    devices_mem = lax.axis_size("mem")
    devices_head = lax.axis_size("head")
    rows, heads, depth = queries.shape
    blocks = cache_blocks.shape[0]
    width = heads * depth
    all_blocks = devices_mem * blocks
    vmem = pl.BlockSpec(memory_space=pltpu.VMEM)
    hbm = pl.BlockSpec(memory_space=pltpu.HBM)
    keep = functools.partial(pltpu.with_memory_space_constraint, memory_space=pltpu.HBM)
    payload = pl.pallas_call(
        payload_kernel,
        in_specs=[hbm] * 2,
        out_specs=vmem,
        out_shape=jax.ShapeDtypeStruct((rows, width + all_blocks), jnp.bfloat16),
        scratch_shapes=[
            pltpu.VMEM(queries.shape, queries.dtype),
            pltpu.VMEM(selected.shape, selected.dtype),
            pltpu.SemaphoreType.DMA((2,)),
        ],
        compiler_params=pltpu.CompilerParams(vmem_limit_bytes=4 * 2**20),
        name="payload",
    )(keep(queries), keep(selected))

    def call(kernel, operands, specs, shapes, limit, scratch=()):
        return pl.pallas_call(
            kernel,
            in_specs=specs,
            out_specs=[vmem] * len(shapes),
            out_shape=shapes,
            scratch_shapes=list(scratch),
            compiler_params=pltpu.CompilerParams(vmem_limit_bytes=limit * 2**20),
        )(*operands)

    def stage(array, after):
        shape = jax.ShapeDtypeStruct(array.shape, array.dtype)
        operands = (keep(array), after)
        sem = [pltpu.SemaphoreType.DMA(())]
        return call(stage_kernel, operands, [hbm, vmem], [shape], 4, sem)[0]

    even = list(range(devices_mem - 2, 0, -2))
    straight = jnp.stack([exchange(payload, "mem", k) for k in even])
    near = exchange(payload, "mem", 1)
    cache_blocks = stage(cache_blocks, payload)
    forwarded = exchange(straight, "mem", 1)
    message = jax.ShapeDtypeStruct((rows, width + LANES), jnp.bfloat16)
    messages = jax.ShapeDtypeStruct((len(even) + 1,) + message.shape, message.dtype)
    hits = jax.ShapeDtypeStruct((1, LANES), jnp.float32)
    attend = functools.partial(attend_kernel, heads=heads)
    mine, hits_a = call(attend, (payload, straight, cache_blocks), [vmem] * 3, [messages, hits], 24)
    theirs, hits_b = call(attend, (near, forwarded, cache_blocks), [vmem] * 3, [messages, hits], 24)
    crossed = exchange(theirs, "mem", 1)
    output_weight = stage(output_weight, theirs)
    merged = call(
        functools.partial(merge_kernel, heads=heads),
        (mine, crossed),
        [vmem] * 2,
        [message] * (len(even) + 1),
        8,
    )
    returned = [merged[0]] + [exchange(m, "mem", k) for k, m in zip(even, merged[1:])]
    share = jax.ShapeDtypeStruct((rows, output_weight.shape[1] // devices_head), jnp.bfloat16)
    far_steps = tuple(range(devices_head - 1, 1, -1))
    near_steps = (1, 0)
    attended, *far = call(
        functools.partial(
            project_far_kernel, sources=len(returned), heads=heads, steps=far_steps
        ),
        (*returned, output_weight),
        [vmem] * (len(returned) + 1),
        [jax.ShapeDtypeStruct((rows, width), jnp.bfloat16)] + [share] * len(far_steps),
        16,
    )
    arrived = {k: exchange(s, "head", k) for k, s in zip(far_steps, far)}
    beside, own = call(
        functools.partial(project_near_kernel, steps=near_steps),
        (attended, output_weight),
        [vmem] * 2,
        [share] * 2,
        16,
    )
    arrived[1] = exchange(beside, "head", 1)
    layer_out = own.astype(jnp.float32)
    for k in range(1, devices_head):
        layer_out = layer_out + arrived[k].astype(jnp.float32)
    decays = 0.5 ** jnp.arange(counts.shape[0], dtype=jnp.float32)
    block_heat = jnp.sum(decays[:, None] * counts.astype(jnp.float32), axis=0) + (hits_a + hits_b)[0, :blocks]
    return (layer_out.astype(jnp.bfloat16), block_heat)


def solution(mesh):
    return jax.shard_map(
        per_device,
        mesh=mesh,
        in_specs=(
            P("mem", "head", None),
            P("mem", None, "head", None, None),
            P("mem", None),
            P(None, "mem"),
            P("head", None),
        ),
        out_specs=(P("mem", "head"), P("mem")),
        check_vma=False,
    )
```

```python
import functools
import math

import jax
import jax.numpy as jnp
from jax import lax
from jax.experimental import pallas as pl
from jax.experimental.pallas import tpu as pltpu
from jax.sharding import PartitionSpec as P


MASKED = -1e30
LANES = 128


def exchange(value, axis, step):
    count = lax.axis_size(axis)
    return lax.ppermute(value, axis, [(i, i ^ step) for i in range(count)])


def even_steps(count):
    half = count // 2
    return [half] + [k for k in range(count - 2, 0, -2) if k != half]


def split_stats(stats, heads):
    high = stats.astype(jnp.bfloat16).astype(jnp.float32)
    rest = stats - high
    middle = rest.astype(jnp.bfloat16).astype(jnp.float32)
    low = rest - middle
    packed = high + pltpu.roll(middle, 2 * heads, 1) + pltpu.roll(low, 4 * heads, 1)
    return packed.astype(jnp.bfloat16)


def join_stats(packed, heads):
    packed = packed.astype(jnp.float32)
    return (
        packed
        + pltpu.roll(packed, LANES - 2 * heads, 1)
        + pltpu.roll(packed, LANES - 4 * heads, 1)
    )


def merge_partials(messages, heads, width):
    depth = width // heads
    scale = depth**-0.5 * math.log2(math.e)
    stats = [join_stats(m[:, width:], heads) for m in messages]
    lane = lax.broadcasted_iota(jnp.int32, stats[0].shape, 1)
    highest = functools.reduce(jnp.maximum, stats)
    factors = [jnp.where(lane < heads, jnp.exp2((s - highest) * scale), 0.0) for s in stats]
    total = sum(f * pltpu.roll(s, LANES - heads, 1) for f, s in zip(factors, stats))
    return highest, total, factors, lane


def weighted_sums(messages, factors, heads, depth):
    for h in range(heads):
        acc = None
        for f, m in zip(factors, messages):
            term = f[:, h : h + 1] * m[:, h * depth : (h + 1) * depth].astype(jnp.float32)
            acc = term if acc is None else acc + term
        yield h, acc.astype(jnp.bfloat16)


def payload_kernel(
    queries_hbm, selected_hbm, out_ref, queries_ref, selected_ref, sems, *, owners, all_blocks
):
    copies = [
        pltpu.make_async_copy(selected_hbm, selected_ref, sems.at[0]),
        pltpu.make_async_copy(queries_hbm, queries_ref, sems.at[1]),
    ]
    for copy in copies:
        copy.start()
    rows, heads, depth = queries_ref.shape
    width = heads * depth
    blocks = all_blocks // owners
    copies[0].wait()
    chosen = selected_ref[...]
    owner = jnp.zeros(chosen.shape, jnp.int32)
    for m in range(1, owners):
        owner = owner + (chosen >= m * blocks).astype(jnp.int32)
    local = chosen - owner * blocks
    fill = jnp.full((rows, LANES - 2 * chosen.shape[1]), -1, jnp.int32)
    tags = jnp.concatenate([owner, local, fill], axis=1)
    out_ref[:, width:] = tags.astype(jnp.float32).astype(jnp.bfloat16)
    copies[1].wait()
    for h in range(heads):
        out_ref[:, h * depth : (h + 1) * depth] = queries_ref[:, h, :]


def stage_kernel(source_hbm, _, out_ref, sem):
    copy = pltpu.make_async_copy(source_hbm, out_ref, sem)
    copy.start()
    copy.wait()


def stage_columns_kernel(weight_hbm, _, *refs, steps):
    outs = refs[:-1]
    me = lax.axis_index("head")
    columns = outs[0].shape[1]
    copies = []
    for i, (k, out) in enumerate(zip(steps, outs)):
        at = pl.multiple_of((me ^ k) * columns, columns)
        copies.append(
            pltpu.make_async_copy(weight_hbm.at[:, pl.ds(at, columns)], out, refs[-1].at[i])
        )
    for copy in copies:
        copy.start()
    for copy in copies:
        copy.wait()


def attend_kernel(
    single_ref, several_ref, cache_ref, first_ref, others_ref, hits_ref, *, heads, picks
):
    blocks, _, heads_kv, tokens, depth = cache_ref.shape
    width = heads * depth
    rows_each = single_ref.shape[0]
    group_q = heads // heads_kv
    scale = depth**-0.5 * math.log2(math.e)
    payloads = [single_ref] + [several_ref.at[i] for i in range(several_ref.shape[0])]
    messages = [first_ref] + [others_ref.at[i] for i in range(others_ref.shape[0])]
    me = lax.axis_index("mem").astype(jnp.float32)
    span = blocks * tokens
    fence = jnp.where(
        lax.broadcasted_iota(jnp.int32, (span, LANES), 0) // tokens
        == lax.broadcasted_iota(jnp.int32, (span, LANES), 1),
        MASKED,
        0.0,
    ).astype(jnp.bfloat16)
    hits = jnp.zeros((1, LANES), jnp.float32)
    batch = min(len(payloads), 8)
    rows = batch * rows_each
    pair = math.gcd(group_q, max(1, 256 // rows))
    lane = lax.broadcasted_iota(jnp.int32, (rows, LANES), 1)
    blocked = []
    for start in range(0, len(payloads), batch):
        tags = jnp.concatenate([p[:, width:] for p in payloads[start : start + batch]], axis=0)
        tags = tags.astype(jnp.float32)
        local = jnp.where(tags == me, pltpu.roll(tags, LANES - picks, 1), -1.0)
        chosen = jnp.zeros((rows, LANES), jnp.float32)
        for i in range(picks):
            chosen = jnp.where(local[:, i : i + 1] == lane.astype(jnp.float32), 1.0, chosen)
        hits = hits + jnp.sum(chosen, axis=0, keepdims=True)
        blocked.append((1.0 - chosen).astype(jnp.bfloat16))
    hits_ref[...] = hits

    def scores_of(start, kv, first_head):
        part = payloads[start : start + batch]
        keys = jnp.concatenate([cache_ref[:, 0, kv].reshape(span, depth), fence], axis=1)
        stacked = []
        for h in range(first_head, first_head + pair):
            query = jnp.concatenate([p[:, h * depth : (h + 1) * depth] for p in part], axis=0)
            stacked.append(jnp.concatenate([query, blocked[start // batch]], axis=1))
        query = jnp.concatenate(stacked, axis=0)
        return lax.dot_general(
            query, keys, (((1,), (1,)), ((), ())), preferred_element_type=jnp.float32
        )

    units = [
        (start, kv, first_head)
        for start in range(0, len(payloads), batch)
        for kv in range(heads_kv)
        for first_head in range(kv * group_q, (kv + 1) * group_q, pair)
    ]
    ahead = scores_of(*units[0])
    stats = None
    for n, (start, kv, first_head) in enumerate(units):
        scores = ahead
        if n + 1 < len(units):
            ahead = scores_of(*units[n + 1])
        values = cache_ref[:, 1, kv].reshape(span, depth)
        values = jnp.concatenate([values, jnp.ones((span, LANES), jnp.bfloat16)], axis=1)
        peak = jnp.max(scores, axis=1, keepdims=True)
        weights = jnp.exp2((scores - peak) * scale).astype(jnp.bfloat16)
        sums = jnp.dot(weights, values, preferred_element_type=jnp.float32)
        out = sums[:, :depth].astype(jnp.bfloat16)
        total = sums[:, depth : depth + 1]
        if first_head == 0:
            stats = jnp.zeros((rows, LANES), jnp.float32)
        for j in range(pair):
            h = first_head + j
            for i in range(batch):
                at = j * rows + i * rows_each
                messages[start + i][:, h * depth : (h + 1) * depth] = out[at : at + rows_each]
            stats = jnp.where(lane == h, peak[j * rows : (j + 1) * rows], stats)
            stats = jnp.where(lane == heads + h, total[j * rows : (j + 1) * rows], stats)
        if first_head + pair == heads:
            packed = split_stats(stats, heads)
            for i in range(batch):
                messages[start + i][:, width:] = packed[i * rows_each : (i + 1) * rows_each]


def merge_kernel(mine_ref, theirs_ref, *outs, heads):
    width = mine_ref.shape[2] - LANES
    depth = width // heads
    for i, out in enumerate(outs):
        pair = [mine_ref.at[i], theirs_ref.at[i]]
        highest, total, factors, lane = merge_partials(pair, heads, width)
        for h, merged in weighted_sums(pair, factors, heads, depth):
            out[:, h * depth : (h + 1) * depth] = merged
        stats = jnp.where(lane < heads, highest, pltpu.roll(total, heads, 1))
        stats = jnp.where(lane < 2 * heads, stats, 0.0)
        out[:, width:] = split_stats(stats, heads)


def project(attended, weights, outs):
    for weight_ref, out in zip(weights, outs):
        out[...] = jnp.dot(
            attended, weight_ref[...], preferred_element_type=jnp.float32
        ).astype(jnp.bfloat16)


def project_far_kernel(*refs, sources, parts, heads):
    messages = refs[:sources]
    weights = refs[sources : sources + parts]
    attended_ref = refs[sources + parts]
    width = attended_ref.shape[1]
    depth = width // heads
    _, total, factors, lane = merge_partials(messages, heads, width)
    inverse = 1.0 / jnp.where(lane < heads, total, 1.0)
    factors = [f * inverse for f in factors]
    attended = jnp.concatenate(
        [a for _, a in weighted_sums(messages, factors, heads, depth)], axis=1
    )
    attended_ref[...] = attended
    project(attended, weights, refs[sources + parts + 1 :])


def project_near_kernel(attended_ref, *refs):
    parts = len(refs) // 2
    project(attended_ref[...], refs[:parts], refs[parts:])


def per_device(queries, cache_blocks, selected, counts, output_weight):
    devices_mem = lax.axis_size("mem")
    devices_head = lax.axis_size("head")
    rows, heads, depth = queries.shape
    blocks = cache_blocks.shape[0]
    picks = selected.shape[1]
    width = heads * depth
    message = jax.ShapeDtypeStruct((rows, width + LANES), jnp.bfloat16)
    vmem = pl.BlockSpec(memory_space=pltpu.VMEM)
    hbm = pl.BlockSpec(memory_space=pltpu.HBM)
    keep = functools.partial(pltpu.with_memory_space_constraint, memory_space=pltpu.HBM)
    payload = pl.pallas_call(
        functools.partial(
            payload_kernel, owners=devices_mem, all_blocks=devices_mem * blocks
        ),
        in_specs=[hbm] * 2,
        out_specs=vmem,
        out_shape=message,
        scratch_shapes=[
            pltpu.VMEM(queries.shape, queries.dtype),
            pltpu.VMEM(selected.shape, selected.dtype),
            pltpu.SemaphoreType.DMA((2,)),
        ],
        compiler_params=pltpu.CompilerParams(vmem_limit_bytes=4 * 2**20),
        name="payload",
    )(keep(queries), keep(selected))

    def call(kernel, operands, specs, shapes, limit, scratch=()):
        return pl.pallas_call(
            kernel,
            in_specs=specs,
            out_specs=[vmem] * len(shapes),
            out_shape=shapes,
            scratch_shapes=list(scratch),
            compiler_params=pltpu.CompilerParams(vmem_limit_bytes=limit * 2**20),
        )(*operands)

    def stage(array, after):
        shape = jax.ShapeDtypeStruct(array.shape, array.dtype)
        operands = (keep(array), after)
        sem = [pltpu.SemaphoreType.DMA(())]
        return call(stage_kernel, operands, [hbm, vmem], [shape], 4, sem)[0]

    even = even_steps(devices_mem)
    straight = jnp.stack([exchange(payload, "mem", k) for k in even])
    near = exchange(payload, "mem", 1)
    cache_blocks = stage(cache_blocks, payload)
    forwarded = exchange(straight, "mem", 1)
    several = jax.ShapeDtypeStruct(straight.shape, straight.dtype)
    hits = jax.ShapeDtypeStruct((1, LANES), jnp.float32)
    attend = functools.partial(attend_kernel, heads=heads, picks=picks)
    own, mine, hits_a = call(
        attend, (payload, straight, cache_blocks), [vmem] * 3, [message, several, hits], 24
    )
    beside, theirs, hits_b = call(
        attend, (near, forwarded, cache_blocks), [vmem] * 3, [message, several, hits], 24
    )
    crossed = exchange(theirs, "mem", 1)
    far_steps = tuple(range(devices_head - 1, 1, -1))
    near_steps = (1, 0)
    columns = output_weight.shape[1] // devices_head
    part = jax.ShapeDtypeStruct((output_weight.shape[0], columns), output_weight.dtype)

    def stage_columns(steps, after):
        return call(
            functools.partial(stage_columns_kernel, steps=steps),
            (keep(output_weight), after),
            [hbm, vmem],
            [part] * len(steps),
            4,
            [pltpu.SemaphoreType.DMA((len(steps),))],
        )

    weight_far = stage_columns(far_steps, theirs)
    merged = call(
        functools.partial(merge_kernel, heads=heads),
        (mine, crossed),
        [vmem] * 2,
        [message] * len(even),
        8,
    )
    returned = [own] + [exchange(m, "mem", k) for k, m in zip(even, merged)]
    returned.append(exchange(beside, "mem", 1))
    weight_near = stage_columns(near_steps, merged[0])
    share = jax.ShapeDtypeStruct((rows, columns), jnp.bfloat16)
    attended, *far = call(
        functools.partial(
            project_far_kernel, sources=len(returned), parts=len(far_steps), heads=heads
        ),
        (*returned, *weight_far),
        [vmem] * (len(returned) + len(far_steps)),
        [jax.ShapeDtypeStruct((rows, width), jnp.bfloat16)] + [share] * len(far_steps),
        16,
    )
    arrived = {k: exchange(s, "head", k) for k, s in zip(far_steps, far)}
    beside, own = call(project_near_kernel, (attended, *weight_near), [vmem] * 3, [share] * 2, 16)
    arrived[1] = exchange(beside, "head", 1)
    layer_out = own.astype(jnp.float32)
    for k in range(1, devices_head):
        layer_out = layer_out + arrived[k].astype(jnp.float32)
    decays = 0.5 ** jnp.arange(counts.shape[0], dtype=jnp.float32)
    block_heat = jnp.sum(decays[:, None] * counts.astype(jnp.float32), axis=0) + (hits_a + hits_b)[0, :blocks]
    return (layer_out.astype(jnp.bfloat16), block_heat)


def solution(mesh):
    return jax.shard_map(
        per_device,
        mesh=mesh,
        in_specs=(
            P("mem", "head", None),
            P("mem", None, "head", None, None),
            P("mem", None),
            P(None, "mem"),
            P("head", None),
        ),
        out_specs=(P("mem", "head"), P("mem")),
        check_vma=False,
    )
```

```python
import functools
import math

import jax
import jax.numpy as jnp
from jax import lax
from jax.experimental import pallas as pl
from jax.experimental.pallas import tpu as pltpu
from jax.sharding import PartitionSpec as P


MASKED = -1e30
LANES = 128


def exchange(value, axis, step):
    count = lax.axis_size(axis)
    return lax.ppermute(value, axis, [(i, i ^ step) for i in range(count)])


def even_steps(count):
    half = count // 2
    return [half] + [k for k in range(count - 2, 0, -2) if k != half]


def split_stats(stats, heads):
    high = stats.astype(jnp.bfloat16).astype(jnp.float32)
    rest = stats - high
    middle = rest.astype(jnp.bfloat16).astype(jnp.float32)
    low = rest - middle
    packed = high + pltpu.roll(middle, 2 * heads, 1) + pltpu.roll(low, 4 * heads, 1)
    return packed.astype(jnp.bfloat16)


def join_stats(packed, heads):
    packed = packed.astype(jnp.float32)
    return (
        packed
        + pltpu.roll(packed, LANES - 2 * heads, 1)
        + pltpu.roll(packed, LANES - 4 * heads, 1)
    )


def merge_partials(messages, heads, width):
    depth = width // heads
    scale = depth**-0.5 * math.log2(math.e)
    stats = [join_stats(m[:, width:], heads) for m in messages]
    lane = lax.broadcasted_iota(jnp.int32, stats[0].shape, 1)
    highest = functools.reduce(jnp.maximum, stats)
    factors = [jnp.where(lane < heads, jnp.exp2((s - highest) * scale), 0.0) for s in stats]
    total = sum(f * pltpu.roll(s, LANES - heads, 1) for f, s in zip(factors, stats))
    return highest, total, factors, lane


def weighted_sums(messages, factors, heads, depth):
    for h in range(heads):
        acc = None
        for f, m in zip(factors, messages):
            term = f[:, h : h + 1] * m[:, h * depth : (h + 1) * depth].astype(jnp.float32)
            acc = term if acc is None else acc + term
        yield h, acc.astype(jnp.bfloat16)


def payload_kernel(
    queries_hbm, selected_hbm, out_ref, queries_ref, selected_ref, sems, *, owners, all_blocks
):
    copies = [
        pltpu.make_async_copy(selected_hbm, selected_ref, sems.at[0]),
        pltpu.make_async_copy(queries_hbm, queries_ref, sems.at[1]),
    ]
    for copy in copies:
        copy.start()
    rows, heads, depth = queries_ref.shape
    width = heads * depth
    blocks = all_blocks // owners
    copies[0].wait()
    chosen = selected_ref[...]
    owner = jnp.zeros(chosen.shape, jnp.int32)
    for m in range(1, owners):
        owner = owner + (chosen >= m * blocks).astype(jnp.int32)
    local = chosen - owner * blocks
    fill = jnp.full((rows, LANES - 2 * chosen.shape[1]), -1, jnp.int32)
    tags = jnp.concatenate([owner, local, fill], axis=1)
    out_ref[:, width:] = tags.astype(jnp.float32).astype(jnp.bfloat16)
    copies[1].wait()
    for h in range(heads):
        out_ref[:, h * depth : (h + 1) * depth] = queries_ref[:, h, :]


def stage_kernel(source_hbm, _, out_ref, sem):
    copy = pltpu.make_async_copy(source_hbm, out_ref, sem)
    copy.start()
    copy.wait()


def stage_columns_kernel(weight_hbm, _, *refs, steps):
    outs = refs[:-1]
    me = lax.axis_index("head")
    columns = outs[0].shape[1]
    copies = []
    for i, (k, out) in enumerate(zip(steps, outs)):
        at = pl.multiple_of((me ^ k) * columns, columns)
        copies.append(
            pltpu.make_async_copy(weight_hbm.at[:, pl.ds(at, columns)], out, refs[-1].at[i])
        )
    for copy in copies:
        copy.start()
    for copy in copies:
        copy.wait()


def attend_kernel(*refs, singles, heads, picks, export):
    several_ref, cache_ref = refs[singles : singles + 2]
    if export:
        *outs, others_ref, hits_ref, keys_ref = refs[singles + 2 :]
    else:
        keys_ref, *outs, others_ref, hits_ref = refs[singles + 2 :]
    blocks, _, heads_kv, tokens, depth = cache_ref.shape
    width = heads * depth
    rows_each = several_ref.shape[1]
    group_q = heads // heads_kv
    scale = depth**-0.5 * math.log2(math.e)
    payloads = list(refs[:singles]) + [several_ref.at[i] for i in range(several_ref.shape[0])]
    messages = outs + [others_ref.at[i] for i in range(others_ref.shape[0])]
    me = lax.axis_index("mem").astype(jnp.float32)
    span = blocks * tokens
    if export:
        fence = jnp.where(
            lax.broadcasted_iota(jnp.int32, (span, LANES), 0) // tokens
            == lax.broadcasted_iota(jnp.int32, (span, LANES), 1),
            MASKED,
            0.0,
        ).astype(jnp.bfloat16)
        for kv in range(heads_kv):
            keys = cache_ref[:, 0, kv].reshape(span, depth)
            keys_ref[kv] = jnp.concatenate([keys, fence], axis=1).T
    hits = jnp.zeros((1, LANES), jnp.float32)
    batches = [payloads[i : i + 8] for i in range(0, len(payloads), 8)]
    blocked = []
    for part in batches:
        tags = jnp.concatenate([p[:, width:] for p in part], axis=0).astype(jnp.float32)
        lane = lax.broadcasted_iota(jnp.int32, tags.shape, 1).astype(jnp.float32)
        local = jnp.where(tags == me, pltpu.roll(tags, LANES - picks, 1), -1.0)
        chosen = jnp.zeros(tags.shape, jnp.float32)
        for i in range(picks):
            chosen = jnp.where(local[:, i : i + 1] == lane, 1.0, chosen)
        hits = hits + jnp.sum(chosen, axis=0, keepdims=True)
        blocked.append((1.0 - chosen).astype(jnp.bfloat16))
    hits_ref[...] = hits

    def scores_of(b, kv, first_head, pair):
        stacked = []
        for h in range(first_head, first_head + pair):
            query = jnp.concatenate(
                [p[:, h * depth : (h + 1) * depth] for p in batches[b]], axis=0
            )
            stacked.append(jnp.concatenate([query, blocked[b]], axis=1))
        query = jnp.concatenate(stacked, axis=0)
        return jnp.dot(query, keys_ref[kv], preferred_element_type=jnp.float32)

    units = []
    for b, part in enumerate(batches):
        pair = group_q if len(part) * rows_each <= 96 else math.gcd(group_q, 2)
        for kv in range(heads_kv):
            for first_head in range(kv * group_q, (kv + 1) * group_q, pair):
                units.append((b, kv, first_head, pair))
    ahead = scores_of(*units[0])
    stats = None
    for n, (b, kv, first_head, pair) in enumerate(units):
        scores = ahead
        if n + 1 < len(units):
            ahead = scores_of(*units[n + 1])
        values = cache_ref[:, 1, kv].reshape(span, depth)
        values = jnp.concatenate([values, jnp.ones((span, LANES), jnp.bfloat16)], axis=1)
        peak = jnp.max(scores, axis=1, keepdims=True)
        weights = jnp.exp2((scores - peak) * scale).astype(jnp.bfloat16)
        sums = jnp.dot(weights, values, preferred_element_type=jnp.float32)
        out = sums[:, :depth].astype(jnp.bfloat16)
        total = sums[:, depth : depth + 1]
        rows = len(batches[b]) * rows_each
        lane = lax.broadcasted_iota(jnp.int32, (rows, LANES), 1)
        if first_head == 0:
            stats = jnp.zeros((rows, LANES), jnp.float32)
        for j in range(pair):
            h = first_head + j
            for i in range(len(batches[b])):
                at = j * rows + i * rows_each
                messages[8 * b + i][:, h * depth : (h + 1) * depth] = out[at : at + rows_each]
            stats = jnp.where(lane == h, peak[j * rows : (j + 1) * rows], stats)
            stats = jnp.where(lane == heads + h, total[j * rows : (j + 1) * rows], stats)
        if first_head + pair == heads:
            packed = split_stats(stats, heads)
            for i in range(len(batches[b])):
                messages[8 * b + i][:, width:] = packed[i * rows_each : (i + 1) * rows_each]


def merge_kernel(mine_ref, theirs_ref, *outs, heads):
    width = mine_ref.shape[2] - LANES
    depth = width // heads
    for i, out in enumerate(outs):
        pair = [mine_ref.at[i], theirs_ref.at[i]]
        highest, total, factors, lane = merge_partials(pair, heads, width)
        for h, merged in weighted_sums(pair, factors, heads, depth):
            out[:, h * depth : (h + 1) * depth] = merged
        stats = jnp.where(lane < heads, highest, pltpu.roll(total, heads, 1))
        stats = jnp.where(lane < 2 * heads, stats, 0.0)
        out[:, width:] = split_stats(stats, heads)


def project(attended, weights, outs):
    for weight_ref, out in zip(weights, outs):
        out[...] = jnp.dot(
            attended, weight_ref[...], preferred_element_type=jnp.float32
        ).astype(jnp.bfloat16)


def project_far_kernel(*refs, sources, parts, heads):
    messages = refs[:sources]
    weights = refs[sources : sources + parts]
    attended_ref = refs[sources + parts]
    width = attended_ref.shape[1]
    depth = width // heads
    _, total, factors, lane = merge_partials(messages, heads, width)
    inverse = 1.0 / jnp.where(lane < heads, total, 1.0)
    factors = [f * inverse for f in factors]
    attended = jnp.concatenate(
        [a for _, a in weighted_sums(messages, factors, heads, depth)], axis=1
    )
    attended_ref[...] = attended
    project(attended, weights, refs[sources + parts + 1 :])


def project_near_kernel(attended_ref, *refs):
    parts = len(refs) // 2
    project(attended_ref[...], refs[:parts], refs[parts:])


def per_device(queries, cache_blocks, selected, counts, output_weight):
    devices_mem = lax.axis_size("mem")
    devices_head = lax.axis_size("head")
    rows, heads, depth = queries.shape
    blocks = cache_blocks.shape[0]
    picks = selected.shape[1]
    width = heads * depth
    message = jax.ShapeDtypeStruct((rows, width + LANES), jnp.bfloat16)
    vmem = pl.BlockSpec(memory_space=pltpu.VMEM)
    hbm = pl.BlockSpec(memory_space=pltpu.HBM)
    keep = functools.partial(pltpu.with_memory_space_constraint, memory_space=pltpu.HBM)
    payload = pl.pallas_call(
        functools.partial(
            payload_kernel, owners=devices_mem, all_blocks=devices_mem * blocks
        ),
        in_specs=[hbm] * 2,
        out_specs=vmem,
        out_shape=message,
        scratch_shapes=[
            pltpu.VMEM(queries.shape, queries.dtype),
            pltpu.VMEM(selected.shape, selected.dtype),
            pltpu.SemaphoreType.DMA((2,)),
        ],
        compiler_params=pltpu.CompilerParams(vmem_limit_bytes=4 * 2**20),
        name="payload",
    )(keep(queries), keep(selected))

    def call(kernel, operands, specs, shapes, limit, scratch=()):
        return pl.pallas_call(
            kernel,
            in_specs=specs,
            out_specs=[vmem] * len(shapes),
            out_shape=shapes,
            scratch_shapes=list(scratch),
            compiler_params=pltpu.CompilerParams(vmem_limit_bytes=limit * 2**20),
        )(*operands)

    def stage(array, after):
        shape = jax.ShapeDtypeStruct(array.shape, array.dtype)
        operands = (keep(array), after)
        sem = [pltpu.SemaphoreType.DMA(())]
        return call(stage_kernel, operands, [hbm, vmem], [shape], 4, sem)[0]

    even = even_steps(devices_mem)
    straight = jnp.stack([exchange(payload, "mem", k) for k in even])
    near = exchange(payload, "mem", 1)
    cache_blocks = stage(cache_blocks, payload)
    forwarded = exchange(straight, "mem", 1)
    several = jax.ShapeDtypeStruct(straight.shape, straight.dtype)
    hits = jax.ShapeDtypeStruct((1, LANES), jnp.float32)

    keys = jax.ShapeDtypeStruct(
        (cache_blocks.shape[2], depth + LANES, blocks * cache_blocks.shape[3]), jnp.bfloat16
    )

    def attend(single, group, keys_in):
        operands = (*single, group, cache_blocks, *keys_in)
        export = not keys_in
        return call(
            functools.partial(
                attend_kernel, singles=len(single), heads=heads, picks=picks, export=export
            ),
            operands,
            [vmem] * len(operands),
            [message] * len(single) + [several, hits] + [keys] * export,
            24,
        )

    own, beside, mine, hits_a, keys = attend([payload, near], straight, [])
    returned_beside = exchange(beside, "mem", 1)
    theirs, hits_b = attend([], forwarded, [keys])
    crossed = exchange(theirs, "mem", 1)
    far_steps = tuple(range(devices_head - 1, 1, -1))
    near_steps = (1, 0)
    columns = output_weight.shape[1] // devices_head
    part = jax.ShapeDtypeStruct((output_weight.shape[0], columns), output_weight.dtype)

    def stage_columns(steps, after):
        return call(
            functools.partial(stage_columns_kernel, steps=steps),
            (keep(output_weight), after),
            [hbm, vmem],
            [part] * len(steps),
            4,
            [pltpu.SemaphoreType.DMA((len(steps),))],
        )

    weight_far = stage_columns(far_steps, theirs)
    merged = call(
        functools.partial(merge_kernel, heads=heads),
        (mine, crossed),
        [vmem] * 2,
        [message] * len(even),
        8,
    )
    returned = [own] + [exchange(m, "mem", k) for k, m in zip(even, merged)]
    returned.append(returned_beside)
    weight_near = stage_columns(near_steps, merged[0])
    share = jax.ShapeDtypeStruct((rows, columns), jnp.bfloat16)
    attended, *far = call(
        functools.partial(
            project_far_kernel, sources=len(returned), parts=len(far_steps), heads=heads
        ),
        (*returned, *weight_far),
        [vmem] * (len(returned) + len(far_steps)),
        [jax.ShapeDtypeStruct((rows, width), jnp.bfloat16)] + [share] * len(far_steps),
        16,
    )
    arrived = {k: exchange(s, "head", k) for k, s in zip(far_steps, far)}
    beside, own = call(project_near_kernel, (attended, *weight_near), [vmem] * 3, [share] * 2, 16)
    arrived[1] = exchange(beside, "head", 1)
    layer_out = own.astype(jnp.float32)
    for k in range(1, devices_head):
        layer_out = layer_out + arrived[k].astype(jnp.float32)
    decays = 0.5 ** jnp.arange(counts.shape[0], dtype=jnp.float32)
    block_heat = jnp.sum(decays[:, None] * counts.astype(jnp.float32), axis=0) + (hits_a + hits_b)[0, :blocks]
    return (layer_out.astype(jnp.bfloat16), block_heat)


def solution(mesh):
    return jax.shard_map(
        per_device,
        mesh=mesh,
        in_specs=(
            P("mem", "head", None),
            P("mem", None, "head", None, None),
            P("mem", None),
            P(None, "mem"),
            P("head", None),
        ),
        out_specs=(P("mem", "head"), P("mem")),
        check_vma=False,
    )
```

```python
import functools
import math

import jax
import jax.numpy as jnp
from jax import lax
from jax.experimental import pallas as pl
from jax.experimental.pallas import tpu as pltpu
from jax.sharding import PartitionSpec as P


MASKED = -1e30
LANES = 128


def exchange(value, axis, step):
    count = lax.axis_size(axis)
    return lax.ppermute(value, axis, [(i, i ^ step) for i in range(count)])


def even_steps(count):
    half = count // 2
    return [half] + [k for k in range(count - 2, 0, -2) if k != half]


def split_stats(stats, heads):
    high = stats.astype(jnp.bfloat16).astype(jnp.float32)
    rest = stats - high
    middle = rest.astype(jnp.bfloat16).astype(jnp.float32)
    low = rest - middle
    packed = high + pltpu.roll(middle, 2 * heads, 1) + pltpu.roll(low, 4 * heads, 1)
    return packed.astype(jnp.bfloat16)


def join_stats(packed, heads):
    packed = packed.astype(jnp.float32)
    return (
        packed
        + pltpu.roll(packed, LANES - 2 * heads, 1)
        + pltpu.roll(packed, LANES - 4 * heads, 1)
    )


def merge_partials(messages, heads, width):
    depth = width // heads
    scale = depth**-0.5 * math.log2(math.e)
    stats = [join_stats(m[:, width:], heads) for m in messages]
    lane = lax.broadcasted_iota(jnp.int32, stats[0].shape, 1)
    highest = functools.reduce(jnp.maximum, stats)
    factors = [jnp.where(lane < heads, jnp.exp2((s - highest) * scale), 0.0) for s in stats]
    total = sum(f * pltpu.roll(s, LANES - heads, 1) for f, s in zip(factors, stats))
    return highest, total, factors, lane


def weighted_sums(messages, factors, heads, depth):
    for h in range(heads):
        acc = None
        for f, m in zip(factors, messages):
            term = f[:, h : h + 1] * m[:, h * depth : (h + 1) * depth].astype(jnp.float32)
            acc = term if acc is None else acc + term
        yield h, acc.astype(jnp.bfloat16)


def payload_kernel(
    queries_hbm, selected_hbm, out_ref, queries_ref, selected_ref, sems, *, owners, all_blocks
):
    copies = [
        pltpu.make_async_copy(selected_hbm, selected_ref, sems.at[0]),
        pltpu.make_async_copy(queries_hbm, queries_ref, sems.at[1]),
    ]
    for copy in copies:
        copy.start()
    rows, heads, depth = queries_ref.shape
    width = heads * depth
    blocks = all_blocks // owners
    copies[0].wait()
    chosen = selected_ref[...]
    owner = jnp.zeros(chosen.shape, jnp.int32)
    for m in range(1, owners):
        owner = owner + (chosen >= m * blocks).astype(jnp.int32)
    local = chosen - owner * blocks
    fill = jnp.full((rows, LANES - 2 * chosen.shape[1]), -1, jnp.int32)
    tags = jnp.concatenate([owner, local, fill], axis=1)
    out_ref[:, width:] = tags.astype(jnp.float32).astype(jnp.bfloat16)
    copies[1].wait()
    for h in range(heads):
        out_ref[:, h * depth : (h + 1) * depth] = queries_ref[:, h, :]


def stage_kernel(source_hbm, _, out_ref, sem):
    copy = pltpu.make_async_copy(source_hbm, out_ref, sem)
    copy.start()
    copy.wait()


def stage_rows_kernel(weight_hbm, _, out_ref, sem, *, first):
    copy = pltpu.make_async_copy(weight_hbm.at[pl.ds(first, out_ref.shape[0])], out_ref, sem)
    copy.start()
    copy.wait()


def attend_kernel(*refs, singles, heads, picks, export):
    several_ref, cache_ref = refs[singles : singles + 2]
    if export:
        *outs, others_ref, hits_ref, keys_ref = refs[singles + 2 :]
    else:
        keys_ref, *outs, others_ref, hits_ref = refs[singles + 2 :]
    blocks, _, heads_kv, tokens, depth = cache_ref.shape
    width = heads * depth
    rows_each = several_ref.shape[1]
    group_q = heads // heads_kv
    scale = depth**-0.5 * math.log2(math.e)
    payloads = list(refs[:singles]) + [several_ref.at[i] for i in range(several_ref.shape[0])]
    messages = outs + [others_ref.at[i] for i in range(others_ref.shape[0])]
    me = lax.axis_index("mem").astype(jnp.float32)
    span = blocks * tokens
    if export:
        fence = jnp.where(
            lax.broadcasted_iota(jnp.int32, (span, LANES), 0) // tokens
            == lax.broadcasted_iota(jnp.int32, (span, LANES), 1),
            MASKED,
            0.0,
        ).astype(jnp.bfloat16)
        for kv in range(heads_kv):
            keys = cache_ref[:, 0, kv].reshape(span, depth)
            keys_ref[kv] = jnp.concatenate([keys, fence], axis=1).T
    hits = jnp.zeros((1, LANES), jnp.float32)
    batches = [payloads[i : i + 8] for i in range(0, len(payloads), 8)]
    blocked = []
    for part in batches:
        tags = jnp.concatenate([p[:, width:] for p in part], axis=0).astype(jnp.float32)
        lane = lax.broadcasted_iota(jnp.int32, tags.shape, 1).astype(jnp.float32)
        local = jnp.where(tags == me, pltpu.roll(tags, LANES - picks, 1), -1.0)
        chosen = jnp.zeros(tags.shape, jnp.float32)
        for i in range(picks):
            chosen = jnp.where(local[:, i : i + 1] == lane, 1.0, chosen)
        hits = hits + jnp.sum(chosen, axis=0, keepdims=True)
        blocked.append((1.0 - chosen).astype(jnp.bfloat16))
    hits_ref[...] = hits

    def scores_of(b, kv, first_head, pair):
        stacked = []
        for h in range(first_head, first_head + pair):
            query = jnp.concatenate(
                [p[:, h * depth : (h + 1) * depth] for p in batches[b]], axis=0
            )
            stacked.append(jnp.concatenate([query, blocked[b]], axis=1))
        query = jnp.concatenate(stacked, axis=0)
        return jnp.dot(query, keys_ref[kv], preferred_element_type=jnp.float32)

    units = []
    for b, part in enumerate(batches):
        pair = group_q if len(part) * rows_each <= 96 else math.gcd(group_q, 2)
        for kv in range(heads_kv):
            for first_head in range(kv * group_q, (kv + 1) * group_q, pair):
                units.append((b, kv, first_head, pair))
    ahead = scores_of(*units[0])
    stats = None
    for n, (b, kv, first_head, pair) in enumerate(units):
        scores = ahead
        if n + 1 < len(units):
            ahead = scores_of(*units[n + 1])
        values = cache_ref[:, 1, kv].reshape(span, depth)
        values = jnp.concatenate([values, jnp.ones((span, LANES), jnp.bfloat16)], axis=1)
        peak = jnp.max(scores, axis=1, keepdims=True)
        weights = jnp.exp2((scores - peak) * scale).astype(jnp.bfloat16)
        sums = jnp.dot(weights, values, preferred_element_type=jnp.float32)
        out = sums[:, :depth].astype(jnp.bfloat16)
        total = sums[:, depth : depth + 1]
        rows = len(batches[b]) * rows_each
        lane = lax.broadcasted_iota(jnp.int32, (rows, LANES), 1)
        if first_head == 0:
            stats = jnp.zeros((rows, LANES), jnp.float32)
        for j in range(pair):
            h = first_head + j
            for i in range(len(batches[b])):
                at = j * rows + i * rows_each
                messages[8 * b + i][:, h * depth : (h + 1) * depth] = out[at : at + rows_each]
            stats = jnp.where(lane == h, peak[j * rows : (j + 1) * rows], stats)
            stats = jnp.where(lane == heads + h, total[j * rows : (j + 1) * rows], stats)
        if first_head + pair == heads:
            packed = split_stats(stats, heads)
            for i in range(len(batches[b])):
                messages[8 * b + i][:, width:] = packed[i * rows_each : (i + 1) * rows_each]


def merge_kernel(mine_ref, theirs_ref, *outs, heads):
    width = mine_ref.shape[2] - LANES
    depth = width // heads
    for i, out in enumerate(outs):
        pair = [mine_ref.at[i], theirs_ref.at[i]]
        highest, total, factors, lane = merge_partials(pair, heads, width)
        for h, merged in weighted_sums(pair, factors, heads, depth):
            out[:, h * depth : (h + 1) * depth] = merged
        stats = jnp.where(lane < heads, highest, pltpu.roll(total, heads, 1))
        stats = jnp.where(lane < 2 * heads, stats, 0.0)
        out[:, width:] = split_stats(stats, heads)


def project(attended, weights, outs, steps):
    me = lax.axis_index("head")
    half = weights[0].shape[0]
    columns = outs[0].shape[1]
    for k, out in zip(steps, outs):
        at = pl.ds(pl.multiple_of((me ^ k) * columns, columns), columns)
        out[...] = sum(
            jnp.dot(
                attended[:, i * half : (i + 1) * half], w[:, at], preferred_element_type=jnp.float32
            )
            for i, w in enumerate(weights)
        ).astype(jnp.bfloat16)


def project_far_kernel(*refs, sources, heads, steps):
    parts = 2
    messages = refs[:sources]
    weights = refs[sources : sources + parts]
    attended_ref = refs[sources + parts]
    width = attended_ref.shape[1]
    depth = width // heads
    _, total, factors, lane = merge_partials(messages, heads, width)
    inverse = 1.0 / jnp.where(lane < heads, total, 1.0)
    factors = [f * inverse for f in factors]
    attended = jnp.concatenate(
        [a for _, a in weighted_sums(messages, factors, heads, depth)], axis=1
    )
    attended_ref[...] = attended
    project(attended, weights, refs[sources + parts + 1 :], steps)


def project_near_kernel(attended_ref, *refs, steps):
    project(attended_ref[...], refs[:2], refs[2:], steps)


def per_device(queries, cache_blocks, selected, counts, output_weight):
    devices_mem = lax.axis_size("mem")
    devices_head = lax.axis_size("head")
    rows, heads, depth = queries.shape
    blocks = cache_blocks.shape[0]
    picks = selected.shape[1]
    width = heads * depth
    message = jax.ShapeDtypeStruct((rows, width + LANES), jnp.bfloat16)
    vmem = pl.BlockSpec(memory_space=pltpu.VMEM)
    hbm = pl.BlockSpec(memory_space=pltpu.HBM)
    keep = functools.partial(pltpu.with_memory_space_constraint, memory_space=pltpu.HBM)
    payload = pl.pallas_call(
        functools.partial(
            payload_kernel, owners=devices_mem, all_blocks=devices_mem * blocks
        ),
        in_specs=[hbm] * 2,
        out_specs=vmem,
        out_shape=message,
        scratch_shapes=[
            pltpu.VMEM(queries.shape, queries.dtype),
            pltpu.VMEM(selected.shape, selected.dtype),
            pltpu.SemaphoreType.DMA((2,)),
        ],
        compiler_params=pltpu.CompilerParams(vmem_limit_bytes=4 * 2**20),
        name="payload",
    )(keep(queries), keep(selected))

    def call(kernel, operands, specs, shapes, limit, scratch=()):
        return pl.pallas_call(
            kernel,
            in_specs=specs,
            out_specs=[vmem] * len(shapes),
            out_shape=shapes,
            scratch_shapes=list(scratch),
            compiler_params=pltpu.CompilerParams(vmem_limit_bytes=limit * 2**20),
        )(*operands)

    def stage(array, after):
        shape = jax.ShapeDtypeStruct(array.shape, array.dtype)
        operands = (keep(array), after)
        sem = [pltpu.SemaphoreType.DMA(())]
        return call(stage_kernel, operands, [hbm, vmem], [shape], 4, sem)[0]

    even = even_steps(devices_mem)
    straight = jnp.stack([exchange(payload, "mem", k) for k in even])
    near = exchange(payload, "mem", 1)
    cache_blocks = stage(cache_blocks, payload)
    forwarded = exchange(straight, "mem", 1)
    several = jax.ShapeDtypeStruct(straight.shape, straight.dtype)
    hits = jax.ShapeDtypeStruct((1, LANES), jnp.float32)

    keys = jax.ShapeDtypeStruct(
        (cache_blocks.shape[2], depth + LANES, blocks * cache_blocks.shape[3]), jnp.bfloat16
    )

    def attend(single, group, keys_in):
        operands = (*single, group, cache_blocks, *keys_in)
        export = not keys_in
        return call(
            functools.partial(
                attend_kernel, singles=len(single), heads=heads, picks=picks, export=export
            ),
            operands,
            [vmem] * len(operands),
            [message] * len(single) + [several, hits] + [keys] * export,
            24,
        )

    own, beside, mine, hits_a, keys = attend([payload, near], straight, [])
    returned_beside = exchange(beside, "mem", 1)
    theirs, hits_b = attend([], forwarded, [keys])
    crossed = exchange(theirs, "mem", 1)
    far_steps = tuple(range(devices_head - 1, 1, -1))
    near_steps = (1, 0)
    columns = output_weight.shape[1] // devices_head
    half = output_weight.shape[0] // 2
    part = jax.ShapeDtypeStruct((half, output_weight.shape[1]), output_weight.dtype)

    def stage_rows(first, after):
        return call(
            functools.partial(stage_rows_kernel, first=first),
            (keep(output_weight), after),
            [hbm, vmem],
            [part],
            4,
            [pltpu.SemaphoreType.DMA(())],
        )[0]

    weight_far = stage_rows(0, theirs)
    merged = call(
        functools.partial(merge_kernel, heads=heads),
        (mine, crossed),
        [vmem] * 2,
        [message] * len(even),
        8,
    )
    returned = [own] + [exchange(m, "mem", k) for k, m in zip(even, merged)]
    returned.append(returned_beside)
    weight_near = stage_rows(half, merged[0])
    share = jax.ShapeDtypeStruct((rows, columns), jnp.bfloat16)
    attended, *far = call(
        functools.partial(
            project_far_kernel, sources=len(returned), heads=heads, steps=far_steps
        ),
        (*returned, weight_far, weight_near),
        [vmem] * (len(returned) + 2),
        [jax.ShapeDtypeStruct((rows, width), jnp.bfloat16)] + [share] * len(far_steps),
        16,
    )
    arrived = {k: exchange(s, "head", k) for k, s in zip(far_steps, far)}
    beside, own = call(
        functools.partial(project_near_kernel, steps=near_steps),
        (attended, weight_far, weight_near),
        [vmem] * 3,
        [share] * 2,
        16,
    )
    arrived[1] = exchange(beside, "head", 1)
    layer_out = own.astype(jnp.float32)
    for k in range(1, devices_head):
        layer_out = layer_out + arrived[k].astype(jnp.float32)
    decays = 0.5 ** jnp.arange(counts.shape[0], dtype=jnp.float32)
    block_heat = jnp.sum(decays[:, None] * counts.astype(jnp.float32), axis=0) + (hits_a + hits_b)[0, :blocks]
    return (layer_out.astype(jnp.bfloat16), block_heat)


def solution(mesh):
    return jax.shard_map(
        per_device,
        mesh=mesh,
        in_specs=(
            P("mem", "head", None),
            P("mem", None, "head", None, None),
            P("mem", None),
            P(None, "mem"),
            P("head", None),
        ),
        out_specs=(P("mem", "head"), P("mem")),
        check_vma=False,
    )
```

```python
import functools
import math

import jax
import jax.numpy as jnp
from jax import lax
from jax.experimental import pallas as pl
from jax.experimental.pallas import tpu as pltpu
from jax.sharding import PartitionSpec as P


MASKED = -1e30
LANES = 128


def exchange(value, axis, step):
    count = lax.axis_size(axis)
    return lax.ppermute(value, axis, [(i, i ^ step) for i in range(count)])


def even_steps(count):
    half = count // 2
    return [half] + [k for k in range(count - 2, 0, -2) if k != half]


def split_stats(stats, heads):
    high = stats.astype(jnp.bfloat16).astype(jnp.float32)
    rest = stats - high
    middle = rest.astype(jnp.bfloat16).astype(jnp.float32)
    low = rest - middle
    packed = high + pltpu.roll(middle, 2 * heads, 1) + pltpu.roll(low, 4 * heads, 1)
    return packed.astype(jnp.bfloat16)


def join_stats(packed, heads):
    packed = packed.astype(jnp.float32)
    return (
        packed
        + pltpu.roll(packed, LANES - 2 * heads, 1)
        + pltpu.roll(packed, LANES - 4 * heads, 1)
    )


def merge_partials(messages, heads, width):
    depth = width // heads
    scale = depth**-0.5 * math.log2(math.e)
    stats = [join_stats(m[:, width:], heads) for m in messages]
    lane = lax.broadcasted_iota(jnp.int32, stats[0].shape, 1)
    highest = functools.reduce(jnp.maximum, stats)
    factors = [jnp.where(lane < heads, jnp.exp2((s - highest) * scale), 0.0) for s in stats]
    total = sum(f * pltpu.roll(s, LANES - heads, 1) for f, s in zip(factors, stats))
    return highest, total, factors, lane


def weighted_sums(messages, factors, heads, depth):
    for h in range(heads):
        acc = None
        for f, m in zip(factors, messages):
            term = f[:, h : h + 1] * m[:, h * depth : (h + 1) * depth].astype(jnp.float32)
            acc = term if acc is None else acc + term
        yield h, acc.astype(jnp.bfloat16)


def payload_kernel(
    queries_hbm, selected_hbm, out_ref, queries_ref, selected_ref, sems, *, owners, all_blocks
):
    copies = [
        pltpu.make_async_copy(selected_hbm, selected_ref, sems.at[0]),
        pltpu.make_async_copy(queries_hbm, queries_ref, sems.at[1]),
    ]
    for copy in copies:
        copy.start()
    rows, heads, depth = queries_ref.shape
    width = heads * depth
    blocks = all_blocks // owners
    copies[0].wait()
    chosen = selected_ref[...]
    owner = jnp.zeros(chosen.shape, jnp.int32)
    for m in range(1, owners):
        owner = owner + (chosen >= m * blocks).astype(jnp.int32)
    local = chosen - owner * blocks
    fill = jnp.full((rows, LANES - 2 * chosen.shape[1]), -1, jnp.int32)
    tags = jnp.concatenate([owner, local, fill], axis=1)
    out_ref[:, width:] = tags.astype(jnp.float32).astype(jnp.bfloat16)
    copies[1].wait()
    for h in range(heads):
        out_ref[:, h * depth : (h + 1) * depth] = queries_ref[:, h, :]


def stage_kernel(source_hbm, _, out_ref, sem):
    copy = pltpu.make_async_copy(source_hbm, out_ref, sem)
    copy.start()
    copy.wait()


def stage_rows_kernel(weight_hbm, _, out_ref, sem, *, first):
    copy = pltpu.make_async_copy(weight_hbm.at[pl.ds(first, out_ref.shape[0])], out_ref, sem)
    copy.start()
    copy.wait()


def attend_kernel(*refs, singles, heads, picks, export):
    several_ref, cache_ref = refs[singles : singles + 2]
    if export:
        *outs, others_ref, hits_ref, keys_ref = refs[singles + 2 :]
    else:
        keys_ref, *outs, others_ref, hits_ref = refs[singles + 2 :]
    blocks, _, heads_kv, tokens, depth = cache_ref.shape
    width = heads * depth
    rows_each = several_ref.shape[1]
    group_q = heads // heads_kv
    scale = depth**-0.5 * math.log2(math.e)
    payloads = list(refs[:singles]) + [several_ref.at[i] for i in range(several_ref.shape[0])]
    messages = outs + [others_ref.at[i] for i in range(others_ref.shape[0])]
    me = lax.axis_index("mem").astype(jnp.float32)
    span = blocks * tokens
    if export:
        fence = jnp.where(
            lax.broadcasted_iota(jnp.int32, (span, LANES), 0) // tokens
            == lax.broadcasted_iota(jnp.int32, (span, LANES), 1),
            MASKED,
            0.0,
        ).astype(jnp.bfloat16)
        for kv in range(heads_kv):
            keys = cache_ref[:, 0, kv].reshape(span, depth)
            keys_ref[kv] = jnp.concatenate([keys, fence], axis=1).T
    hits = jnp.zeros((1, LANES), jnp.float32)
    batches = [payloads[i : i + 8] for i in range(0, len(payloads), 8)]
    blocked = []
    for part in batches:
        tags = jnp.concatenate([p[:, width:] for p in part], axis=0).astype(jnp.float32)
        lane = lax.broadcasted_iota(jnp.int32, tags.shape, 1).astype(jnp.float32)
        local = jnp.where(tags == me, pltpu.roll(tags, LANES - picks, 1), -1.0)
        chosen = jnp.zeros(tags.shape, jnp.float32)
        for i in range(picks):
            chosen = jnp.where(local[:, i : i + 1] == lane, 1.0, chosen)
        hits = hits + jnp.sum(chosen, axis=0, keepdims=True)
        blocked.append((1.0 - chosen).astype(jnp.bfloat16))
    hits_ref[...] = hits

    def scores_of(b, kv, first_head, pair):
        stacked = []
        for h in range(first_head, first_head + pair):
            query = jnp.concatenate(
                [p[:, h * depth : (h + 1) * depth] for p in batches[b]], axis=0
            )
            stacked.append(jnp.concatenate([query, blocked[b]], axis=1))
        query = jnp.concatenate(stacked, axis=0)
        return jnp.dot(query, keys_ref[kv], preferred_element_type=jnp.float32)

    units = []
    for b, part in enumerate(batches):
        pair = group_q if len(part) * rows_each <= 96 else math.gcd(group_q, 2)
        for kv in range(heads_kv):
            for first_head in range(kv * group_q, (kv + 1) * group_q, pair):
                units.append((b, kv, first_head, pair))
    ahead = scores_of(*units[0])
    stats = None
    for n, (b, kv, first_head, pair) in enumerate(units):
        scores = ahead
        if n + 1 < len(units):
            ahead = scores_of(*units[n + 1])
        values = cache_ref[:, 1, kv].reshape(span, depth)
        values = jnp.concatenate([values, jnp.ones((span, LANES), jnp.bfloat16)], axis=1)
        peak = jnp.max(scores, axis=1, keepdims=True)
        weights = jnp.exp2((scores - peak) * scale).astype(jnp.bfloat16)
        sums = jnp.dot(weights, values, preferred_element_type=jnp.float32)
        out = sums[:, :depth].astype(jnp.bfloat16)
        total = sums[:, depth : depth + 1]
        rows = len(batches[b]) * rows_each
        lane = lax.broadcasted_iota(jnp.int32, (rows, LANES), 1)
        if first_head == 0:
            stats = jnp.zeros((rows, LANES), jnp.float32)
        for j in range(pair):
            h = first_head + j
            for i in range(len(batches[b])):
                at = j * rows + i * rows_each
                messages[8 * b + i][:, h * depth : (h + 1) * depth] = out[at : at + rows_each]
            stats = jnp.where(lane == h, peak[j * rows : (j + 1) * rows], stats)
            stats = jnp.where(lane == heads + h, total[j * rows : (j + 1) * rows], stats)
        if first_head + pair == heads:
            packed = split_stats(stats, heads)
            for i in range(len(batches[b])):
                messages[8 * b + i][:, width:] = packed[i * rows_each : (i + 1) * rows_each]


def merge_kernel(mine_ref, theirs_ref, *outs, heads):
    width = mine_ref.shape[2] - LANES
    depth = width // heads
    for i, out in enumerate(outs):
        pair = [mine_ref.at[i], theirs_ref.at[i]]
        highest, total, factors, lane = merge_partials(pair, heads, width)
        for h, merged in weighted_sums(pair, factors, heads, depth):
            out[:, h * depth : (h + 1) * depth] = merged
        stats = jnp.where(lane < heads, highest, pltpu.roll(total, heads, 1))
        stats = jnp.where(lane < 2 * heads, stats, 0.0)
        out[:, width:] = split_stats(stats, heads)


def project(attended, weights, outs, steps):
    me = lax.axis_index("head")
    half = weights[0].shape[0]
    columns = outs[0].shape[1]
    for k, out in zip(steps, outs):
        at = pl.ds(pl.multiple_of((me ^ k) * columns, columns), columns)
        out[...] = sum(
            jnp.dot(
                attended[:, i * half : (i + 1) * half], w[:, at], preferred_element_type=jnp.float32
            )
            for i, w in enumerate(weights)
        ).astype(jnp.bfloat16)


def project_far_kernel(*refs, sources, heads, steps):
    parts = 2
    messages = refs[:sources]
    weights = refs[sources : sources + parts]
    attended_ref = refs[sources + parts]
    width = attended_ref.shape[1]
    depth = width // heads
    _, total, factors, lane = merge_partials(messages, heads, width)
    inverse = 1.0 / jnp.where(lane < heads, total, 1.0)
    factors = [f * inverse for f in factors]
    attended = jnp.concatenate(
        [a for _, a in weighted_sums(messages, factors, heads, depth)], axis=1
    )
    attended_ref[...] = attended
    project(attended, weights, refs[sources + parts + 1 :], steps)


def project_near_kernel(attended_ref, *refs, steps):
    project(attended_ref[...], refs[:2], refs[2:], steps)


def per_device(queries, cache_blocks, selected, counts, output_weight):
    devices_mem = lax.axis_size("mem")
    devices_head = lax.axis_size("head")
    rows, heads, depth = queries.shape
    blocks = cache_blocks.shape[0]
    picks = selected.shape[1]
    width = heads * depth
    message = jax.ShapeDtypeStruct((rows, width + LANES), jnp.bfloat16)
    vmem = pl.BlockSpec(memory_space=pltpu.VMEM)
    hbm = pl.BlockSpec(memory_space=pltpu.HBM)
    keep = functools.partial(pltpu.with_memory_space_constraint, memory_space=pltpu.HBM)
    payload = pl.pallas_call(
        functools.partial(
            payload_kernel, owners=devices_mem, all_blocks=devices_mem * blocks
        ),
        in_specs=[hbm] * 2,
        out_specs=vmem,
        out_shape=message,
        scratch_shapes=[
            pltpu.VMEM(queries.shape, queries.dtype),
            pltpu.VMEM(selected.shape, selected.dtype),
            pltpu.SemaphoreType.DMA((2,)),
        ],
        compiler_params=pltpu.CompilerParams(vmem_limit_bytes=4 * 2**20),
        name="payload",
    )(keep(queries), keep(selected))

    def call(kernel, operands, specs, shapes, limit, scratch=()):
        return pl.pallas_call(
            kernel,
            in_specs=specs,
            out_specs=[vmem] * len(shapes),
            out_shape=shapes,
            scratch_shapes=list(scratch),
            compiler_params=pltpu.CompilerParams(vmem_limit_bytes=limit * 2**20),
        )(*operands)

    def stage(array, after):
        shape = jax.ShapeDtypeStruct(array.shape, array.dtype)
        operands = (keep(array), after)
        sem = [pltpu.SemaphoreType.DMA(())]
        return call(stage_kernel, operands, [hbm, vmem], [shape], 4, sem)[0]

    even = even_steps(devices_mem)
    straight = jnp.stack([exchange(payload, "mem", k) for k in even])
    near = exchange(payload, "mem", 1)
    cache_blocks = stage(cache_blocks, payload)
    forwarded = exchange(straight, "mem", 1)
    several = jax.ShapeDtypeStruct(straight.shape, straight.dtype)
    hits = jax.ShapeDtypeStruct((1, LANES), jnp.float32)

    keys = jax.ShapeDtypeStruct(
        (cache_blocks.shape[2], depth + LANES, blocks * cache_blocks.shape[3]), jnp.bfloat16
    )

    def attend(single, group, keys_in):
        operands = (*single, group, cache_blocks, *keys_in)
        export = not keys_in
        return call(
            functools.partial(
                attend_kernel, singles=len(single), heads=heads, picks=picks, export=export
            ),
            operands,
            [vmem] * len(operands),
            [message] * len(single) + [several, hits] + [keys] * export,
            24,
        )

    own, beside, mine, hits_a, keys = attend([payload, near], straight, [])
    returned_beside = exchange(beside, "mem", 1)
    theirs, hits_b = attend([], forwarded, [keys])
    crossed = exchange(theirs, "mem", 1)
    far_steps = tuple(range(devices_head - 1, 1, -1))
    near_steps = (1, 0)
    columns = output_weight.shape[1] // devices_head
    half = output_weight.shape[0] // 2
    part = jax.ShapeDtypeStruct((half, output_weight.shape[1]), output_weight.dtype)

    def stage_rows(first, after):
        return call(
            functools.partial(stage_rows_kernel, first=first),
            (keep(output_weight), after),
            [hbm, vmem],
            [part],
            4,
            [pltpu.SemaphoreType.DMA(())],
        )[0]

    weight_far = stage_rows(0, theirs)
    merged = call(
        functools.partial(merge_kernel, heads=heads),
        (mine, crossed),
        [vmem] * 2,
        [message] * len(even),
        8,
    )
    returned = [own] + [exchange(m, "mem", k) for k, m in zip(even, merged)]
    weight_near = stage_rows(half, merged[0])
    (local,) = call(
        functools.partial(merge_kernel, heads=heads),
        (own[None], returned_beside[None]),
        [vmem] * 2,
        [message],
        8,
    )
    returned = [local] + returned[1:]
    share = jax.ShapeDtypeStruct((rows, columns), jnp.bfloat16)
    attended, *far = call(
        functools.partial(
            project_far_kernel, sources=len(returned), heads=heads, steps=far_steps
        ),
        (*returned, weight_far, weight_near),
        [vmem] * (len(returned) + 2),
        [jax.ShapeDtypeStruct((rows, width), jnp.bfloat16)] + [share] * len(far_steps),
        16,
    )
    arrived = {k: exchange(s, "head", k) for k, s in zip(far_steps, far)}
    beside, own = call(
        functools.partial(project_near_kernel, steps=near_steps),
        (attended, weight_far, weight_near),
        [vmem] * 3,
        [share] * 2,
        16,
    )
    arrived[1] = exchange(beside, "head", 1)
    layer_out = own.astype(jnp.float32)
    for k in range(1, devices_head):
        layer_out = layer_out + arrived[k].astype(jnp.float32)
    decays = 0.5 ** jnp.arange(counts.shape[0], dtype=jnp.float32)
    block_heat = jnp.sum(decays[:, None] * counts.astype(jnp.float32), axis=0) + (hits_a + hits_b)[0, :blocks]
    return (layer_out.astype(jnp.bfloat16), block_heat)


def solution(mesh):
    return jax.shard_map(
        per_device,
        mesh=mesh,
        in_specs=(
            P("mem", "head", None),
            P("mem", None, "head", None, None),
            P("mem", None),
            P(None, "mem"),
            P("head", None),
        ),
        out_specs=(P("mem", "head"), P("mem")),
        check_vma=False,
    )
```
